32 devices in a mesh: ctx: 16 (over z, y, core), tp: 2 (over x).
Axes of the slice: x: 2, y: 2, z: 4, core: 2. Of those that a mesh axis runs over, the one named last changes fastest.
Arguments:
- attn_q: bfloat16 [4096, 2048], P('ctx', 'tp'), may hold values from -5 to 5
- attn_k: bfloat16 [4096, 2048], P('ctx', 'tp'), may hold values from -5 to 5
- attn_v: bfloat16 [4096, 2048], P('ctx', 'tp'), may hold values from -6 to 6
- attn_o: bfloat16 [4096, 2048], P('ctx', 'tp'), may hold values from -6 to 6
- attn_dy: bfloat16 [4096, 8192], P('ctx', 'tp'), may hold values from -6 to 6
- out_weight: bfloat16 [2048, 8192], P('tp'), may hold values from -0.0625 to 0.0625
- block_place: int32 [32], replicated, may hold values from 0 to 31, each once
- hyena_q: bfloat16 [4096, 4096], P('ctx', 'tp'), may hold values from -6 to 6
- hyena_k: bfloat16 [4096, 4096], P('ctx', 'tp'), may hold values from -6 to 6
- hyena_v: bfloat16 [4096, 4096], P('ctx', 'tp'), may hold values from -6 to 6
- hyena_dy: bfloat16 [4096, 4096], P('ctx', 'tp'), may hold values from -6 to 6
- filter_residue: float32 [16, 32], P(None, 'tp')
- filter_rate: float32 [16, 32], P(None, 'tp'), as said below
Outputs:
- grad_q_attn: bfloat16 [4096, 2048], P('ctx', 'tp')
- grad_k_attn: bfloat16 [4096, 2048], P('ctx', 'tp')
- grad_v_attn: bfloat16 [4096, 2048], P('ctx', 'tp')
- grad_q_hyena: bfloat16 [4096, 4096], P('ctx', 'tp')
- grad_k_hyena: bfloat16 [4096, 4096], P('ctx', 'tp')
- grad_v_hyena: bfloat16 [4096, 4096], P('ctx', 'tp')
The draws below stay inside these ranges and needn't reach their ends.
Inputs may be any that keep to these rules, and one draw needn't show every extreme that they name: A permutation of the 32 block places; index d of ctx holds, as its 256 rows of every attention array, the blocks at places block_place[2 d] and block_place[2 d + 1], in that order. `filter_rate`: positive, at most 1/30.
All inputs are finite; a program needn't handle non-finite values.
Results may differ from the reference program's by a relative error of at most 0.009.
Values may be sent and summed in bfloat16 or wider, within the bound.
A program may use at most 256 MiB of HBM per device.

```python
import math
import jax
import jax.numpy as jnp
from jax import lax

D = 8192
HD = 128
HEADS = 16
CHAN = 4096
GS = 128
MODES = 16
TOK_DEV = 256
TOKENS = 4096
BLOCKS = 32
N_CTX = 16


def filter_parts(key):
    grid_dims = (MODES, CHAN // GS)
    slow_pick = jax.random.randint(jax.random.fold_in(key, 11), grid_dims, 0, 2) == 1
    mixing = jax.random.uniform(jax.random.fold_in(key, 12), grid_dims, jnp.float32)
    slow_rate = 0.3 / TOKENS * jnp.exp(mixing * math.log(20.0 / 3.0))
    fast_rate = 1.0 / 50.0 * jnp.exp(mixing * math.log(50.0 / 30.0))
    rate_all = jnp.where(slow_pick, slow_rate, fast_rate)
    residue_all = jax.random.normal(jax.random.fold_in(key, 13), grid_dims, jnp.float32) * jnp.sqrt(2.0 * rate_all) * 0.5
    return (rate_all, residue_all)


def draw_filter_rate(key, part):
    return filter_parts(key)[0].astype(jnp.float32)


def draw_filter_residue(key, part):
    return filter_parts(key)[1].astype(jnp.float32)


def base_values(key, salt):
    feat_all = HEADS * HD
    return jnp.clip(jax.random.normal(jax.random.fold_in(key, salt), (TOKENS, feat_all), jnp.float32), -4.5, 4.5)


def draw_attn_q(key, part):
    values_base = base_values(key, 1)
    return values_base.astype(jnp.bfloat16)


def draw_attn_k(key, part):
    values_base = base_values(key, 2)
    return values_base.astype(jnp.bfloat16)


def shard_levels(rng, shape, split, low, largest):
    def one(dim, parts):
        draws = jax.random.uniform(jax.random.fold_in(jax.random.fold_in(rng, 6), dim), (parts,), jnp.float32, low / len(split), largest / len(split))
        return jnp.repeat(jnp.exp(draws), shape[dim] // parts).reshape((-1,) + (1,) * (len(shape) - dim - 1))

    level = one(*split[0])
    for cut in split[1:]:
        level = level * one(*cut)
    return level


def scatter_about(rng, extent, spread, bound, shards=(), kind=jnp.bfloat16):
    result = spread * jax.random.normal(rng, extent, jnp.float32)
    if shards:
        result = result * shard_levels(rng, extent, shards, -0.22, 0.18)
    return jnp.clip(result, -bound, bound).astype(kind)


def setup_inputs(seed: int = 0) -> dict:
    arg_keys = jax.random.split(jax.random.key(seed), 14)
    attn_q = draw_attn_q(jax.random.fold_in(arg_keys[13], 71), 0)
    attn_k = draw_attn_k(jax.random.fold_in(arg_keys[13], 71), 0)
    attn_v = scatter_about(arg_keys[2], (TOKENS, HEADS * HD), 1.0, 6.0, ((0, 16), (1, 2)))
    attn_o = scatter_about(arg_keys[3], (TOKENS, HEADS * HD), 1.0, 6.0, ((0, 16), (1, 2)))
    attn_dy = scatter_about(arg_keys[4], (TOKENS, D), 1.0, 6.0, ((0, 16), (1, 2)))
    out_weight = scatter_about(arg_keys[5], (HEADS * HD, D), D ** -0.5, 0.0625, ((0, 2),))
    block_place = jax.random.permutation(arg_keys[6], BLOCKS).astype(jnp.int32)
    hyena_q = scatter_about(arg_keys[7], (TOKENS, CHAN), 1.0, 6.0, ((0, 16), (1, 2)))
    hyena_k = scatter_about(arg_keys[8], (TOKENS, CHAN), 1.0, 6.0, ((0, 16), (1, 2)))
    hyena_v = scatter_about(arg_keys[9], (TOKENS, CHAN), 1.0, 6.0, ((0, 16), (1, 2)))
    hyena_dy = scatter_about(arg_keys[10], (TOKENS, CHAN), 1.0, 6.0, ((0, 16), (1, 2)))
    filter_residue = draw_filter_residue(jax.random.fold_in(arg_keys[13], 71), 0)
    filter_rate = draw_filter_rate(jax.random.fold_in(arg_keys[13], 71), 0)
    return dict(attn_q=attn_q, attn_k=attn_k, attn_v=attn_v, attn_o=attn_o, attn_dy=attn_dy, out_weight=out_weight, block_place=block_place, hyena_q=hyena_q, hyena_k=hyena_k, hyena_v=hyena_v, hyena_dy=hyena_dy, filter_residue=filter_residue, filter_rate=filter_rate)


def toeplitz_rows(filter_taps):
    groups, block_len = filter_taps.shape
    padded = jnp.concatenate([jnp.zeros_like(filter_taps), filter_taps], axis=1)[:, ::-1]
    flattened = jnp.tile(padded, (1, block_len))[:, :block_len * (2 * block_len - 1)]
    return flattened.reshape(groups, block_len, 2 * block_len - 1)[:, :, block_len - 1:]


def hyena_tables(filter_residue, filter_rate, block_len):
    lag_ids = jnp.arange(block_len).astype(jnp.float32)
    rate_col = filter_rate[:, :, None]
    head_decay = jnp.exp(-rate_col * lag_ids)
    filter_taps = jnp.einsum('mg,mgl->gl', filter_residue, head_decay, precision=lax.Precision.HIGHEST)
    tail_decay = jnp.exp(-rate_col * (block_len - 1 - lag_ids))
    into_block = filter_residue[:, :, None] * jnp.exp(-rate_col * (lag_ids + 1.0))
    back_block = filter_residue[:, :, None] * jnp.exp(-rate_col * (block_len - lag_ids))
    block_decay = jnp.exp(-filter_rate * block_len)
    return toeplitz_rows(filter_taps), tail_decay, head_decay, into_block, back_block, block_decay


def hyena_grads(hyena_q, hyena_k, hyena_v, hyena_dy, filter_residue, filter_rate):
    groups = CHAN // GS
    block_shape = (N_CTX, TOK_DEV, groups, GS)
    prod_kv = (hyena_k.astype(jnp.float32) * hyena_v.astype(jnp.float32)).reshape(block_shape)
    prod_qdy = (hyena_q.astype(jnp.float32) * hyena_dy.astype(jnp.float32)).reshape(block_shape)
    toeplitz, tail_decay, head_decay, into_block, back_block, block_decay = hyena_tables(filter_residue, filter_rate, TOK_DEV)
    decay_col = block_decay[:, :, None]
    highest = lax.Precision.HIGHEST

    def forward_step(state, prod_blk):
        conv = jnp.einsum('gts,sgc->tgc', toeplitz, prod_blk, precision=highest)
        conv = conv + jnp.einsum('mgt,mgc->tgc', into_block, state, precision=highest)
        state = decay_col * state + jnp.einsum('mgs,sgc->mgc', tail_decay, prod_blk, precision=highest)
        return state, conv

    def backward_step(state, prod_blk):
        grad_mid = jnp.einsum('gts,tgc->sgc', toeplitz, prod_blk, precision=highest)
        grad_mid = grad_mid + jnp.einsum('mgs,mgc->sgc', back_block, state, precision=highest)
        state = decay_col * state + jnp.einsum('mgt,tgc->mgc', head_decay, prod_blk, precision=highest)
        return state, grad_mid

    zero_state = jnp.zeros((MODES, groups, GS), jnp.float32)
    _, conv = lax.scan(forward_step, zero_state, prod_kv)
    _, grad_mid = lax.scan(backward_step, zero_state, prod_qdy, reverse=True)
    conv = conv.reshape(TOKENS, CHAN)
    grad_mid = grad_mid.reshape(TOKENS, CHAN)
    grad_q = (hyena_dy.astype(jnp.float32) * conv).astype(jnp.bfloat16)
    grad_k = (grad_mid * hyena_v.astype(jnp.float32)).astype(jnp.bfloat16)
    grad_v = (grad_mid * hyena_k.astype(jnp.float32)).astype(jnp.bfloat16)
    return grad_q, grad_k, grad_v


def attention_grads(attn_q, attn_k, attn_v, attn_o, attn_dy, out_weight, block_place):
    block_len = TOK_DEV // 2
    row_ids = jnp.arange(TOKENS).astype(jnp.int32)
    seq_place = (block_place[row_ids // block_len] * block_len + row_ids % block_len).astype(jnp.int32)
    order_rows = jnp.zeros((TOKENS,), jnp.int32).at[seq_place].set(row_ids)
    grad_out = jnp.dot(attn_dy, out_weight.T, preferred_element_type=jnp.float32).astype(jnp.bfloat16)
    delta = jnp.sum((grad_out.astype(jnp.float32) * attn_o.astype(jnp.float32)).reshape(TOKENS, HEADS, HD), axis=2)

    def ordered(array):
        return array[order_rows].reshape(TOKENS, HEADS, HD).astype(jnp.float32)

    q_seq = ordered(attn_q)
    k_seq = ordered(attn_k)
    v_seq = ordered(attn_v)
    grad_seq = ordered(grad_out)
    delta_seq = delta[order_rows]
    softmax_scale = HD ** -0.5
    block_rows = 4 * TOK_DEV
    grad_q_parts = []
    grad_k_seq = jnp.zeros((TOKENS, HEADS, HD), jnp.float32)
    grad_v_seq = jnp.zeros((TOKENS, HEADS, HD), jnp.float32)
    for block_id in range(TOKENS // block_rows):
        row_start = block_id * block_rows
        row_end = row_start + block_rows
        query_blk = q_seq[row_start:row_end]
        grad_blk = grad_seq[row_start:row_end]
        key_blk = k_seq[:row_end]
        value_blk = v_seq[:row_end]
        scores = jnp.einsum('qhd,khd->hqk', query_blk, key_blk) * softmax_scale
        visible = jnp.arange(row_end)[None, :] <= jnp.arange(row_start, row_end)[:, None]
        scores = jnp.where(visible[None], scores, -jnp.inf)
        row_peak = jnp.max(scores, axis=2, keepdims=True)
        log_total = row_peak + jnp.log(jnp.sum(jnp.exp(scores - row_peak), axis=2, keepdims=True))
        probs_full = jnp.exp(scores - log_total)
        probs_low = lax.optimization_barrier(probs_full.astype(jnp.bfloat16)).astype(jnp.float32)
        grad_prob = jnp.einsum('qhd,khd->hqk', grad_blk, value_blk)
        delta_blk = delta_seq[row_start:row_end].T[:, :, None]
        grad_score = probs_full * (grad_prob - delta_blk)
        grad_score = lax.optimization_barrier(grad_score.astype(jnp.bfloat16)).astype(jnp.float32)
        grad_q_parts.append(jnp.einsum('hqk,khd->qhd', grad_score, key_blk) * softmax_scale)
        grad_k_seq = grad_k_seq.at[:row_end].add(jnp.einsum('hqk,qhd->khd', grad_score, query_blk) * softmax_scale)
        grad_v_seq = grad_v_seq.at[:row_end].add(jnp.einsum('hqk,qhd->khd', probs_low, grad_blk))
    grad_q_seq = jnp.concatenate(grad_q_parts, axis=0)

    def stored(array):
        return array[seq_place].reshape(TOKENS, HEADS * HD).astype(jnp.bfloat16)

    return stored(grad_q_seq), stored(grad_k_seq), stored(grad_v_seq)


def reference(attn_q, attn_k, attn_v, attn_o, attn_dy, out_weight, block_place, hyena_q, hyena_k, hyena_v, hyena_dy, filter_residue, filter_rate):
    attention = attention_grads(attn_q, attn_k, attn_v, attn_o, attn_dy, out_weight, block_place)
    hyena = hyena_grads(hyena_q, hyena_k, hyena_v, hyena_dy, filter_residue, filter_rate)
    return (attention[0], attention[1], attention[2], hyena[0], hyena[1], hyena[2])
```

```python
import functools
import math

import jax
import jax.numpy as jnp
from jax import lax
from jax.experimental import pallas as pl
from jax.experimental.pallas import tpu as pltpu
from jax.sharding import PartitionSpec as P

HD = 128
NEG_LARGE = -1e30
F32 = jnp.float32
BF16 = jnp.bfloat16
MESH = pl.DeviceIdType.MESH
LN2_SCALE = HD ** (-0.5) * math.log2(math.e)
SCALE = HD ** (-0.5)


def dot_nn(a, b):
    return lax.dot_general(a, b, (((1,), (0,)), ((), ())), preferred_element_type=F32)


def dot_nt(a, b):
    return lax.dot_general(a, b, (((1,), (1,)), ((), ())), preferred_element_type=F32)


def split(x):
    high = x.astype(BF16)
    return high, (x - high.astype(F32)).astype(BF16)


def rows_at(block, size):
    return pl.ds(pl.multiple_of(block * size, size), size)


def loop(start, stop, fn):
    def step(i, carry):
        fn(i)
        return carry

    lax.fori_loop(start, stop, step, 0)


class Plan:
    def __init__(self, count, parts, tok, feat, width, chan, modes, groups):
        self.count, self.parts = count, parts
        self.tok, self.feat, self.width = tok, feat, width
        self.chan, self.modes, self.groups = chan, modes, groups
        self.heads = feat // HD
        self.share = count // self.heads
        self.half = tok // 2
        self.near = 4 if count % 4 == 0 else count
        self.far = count // self.near
        self.chunks = 4
        self.piece = tok // self.chunks
        self.tile = min(256, feat)
        self.size = chan // groups
        self.blocks = max(
            sum(count - self.own(n, turn) for n in range(self.heads)) for turn in range(self.share)
        )

    def own(self, n, turn):
        return n * self.share + turn + (n % 2) * (self.share - 1 - 2 * turn)

    def offset(self, n, turn):
        share = self.share
        before = (
            share * (n * (n - 1) // 2) + ((n + 1) // 2) * turn + (n // 2) * (share - 1 - turn)
        )
        return n * self.count - before

    def held(self, i, turn):
        at = i // self.share
        mine = self.own(at, turn) - at * self.share
        return at + (i % self.share - mine + self.share) // self.share


def scratch(p):
    vm = pltpu.VMEM
    total = p.count * p.tok
    low = vm((total, HD), BF16)
    blocked = vm((2 * p.count, p.half, HD), BF16)
    other = max(p.share - 1, 1)
    rest = max(p.parts - 1, 1)
    lines = p.groups * p.modes
    dma = pltpu.SemaphoreType.DMA

    def pair(*shape):
        return [dma(shape), dma(shape)]

    items = dict(
        dy_own=vm((p.tok, p.width), BF16),
        dy_got=vm((rest, p.tok, p.width), BF16),
        w_own=vm((p.feat, p.width), BF16),
        w_rest=vm((rest, p.feat, p.width), BF16),
        g_part=vm((p.tok, p.feat), F32),
        o_buf=vm((p.tok, p.feat), BF16),
        g_low=vm((p.tok, p.feat), BF16),
        delta_out=vm((p.heads, 2, 8, HD), F32),
        delta_all=vm((2 * p.count, 8, HD), F32),
        delta_seq=vm((2 * p.count, 8, HD), F32),
        q_all=blocked,
        k_all=blocked,
        v_all=blocked,
        g_all=blocked,
        q_seq=low,
        k_seq=low,
        v_seq=low,
        g_seq=low,
        k_turn=vm((p.heads, HD, p.tok), BF16),
        cache=vm((p.blocks, p.tok, p.tok), BF16),
        ml=vm((p.heads * p.count, 8, p.tok), F32),
        ml_own=vm((p.count, 8, p.tok), F32),
        ml_got=vm((other, p.count, 8, p.tok), F32),
        dq_seq=vm((2 * p.count, p.half, HD), F32),
        dq_out=vm((other, 2 * p.heads, p.half, HD), F32),
        dq_got=vm((other, 2 * p.heads, p.half, HD), F32),
        dk_seq=blocked,
        dv_seq=blocked,
        send=vm((3, p.heads, 2, p.half, HD), BF16),
        hy_in=vm((4, p.tok, p.chan), BF16),
        hy_out=vm((3, p.tok, p.chan), BF16),
        st_own=vm((2, lines, HD), BF16),
        st_got=vm((p.near, 2, lines, HD), BF16),
        st_far=vm((2, lines, HD), BF16),
        far_got=vm((max(p.far - 1, 1), lines, HD), BF16),
        st_fin=vm((2, lines, HD), F32),
        sem_local=dma((16,)),
        sem_rest=dma((rest,)),
        sem_out=dma((6,)),
        sem_dy_s=dma((rest, p.chunks)),
        sem_dy_r=dma((rest, p.chunks)),
        sem_in_s=dma((3, p.heads)),
        sem_in_r=dma((3, p.heads)),
        sem_fw_s=dma((3, p.share)),
        sem_fw_r=dma((3, p.share)),
        sem_g_s=dma((p.chunks, p.heads)),
        sem_g_r=dma((p.chunks, p.heads)),
        sem_gf_s=dma((p.chunks, p.share)),
        sem_gf_r=dma((p.chunks, p.share)),
        sem_d_s=dma((p.heads,)),
        sem_d_r=dma((p.heads,)),
        sem_df_s=dma((p.share,)),
        sem_df_r=dma((p.share,)),
        sem_st_s=dma((p.near,)),
        sem_st_r=dma((p.near,)),
        sem_far_s=dma((p.far,)),
        sem_far_r=dma((p.far,)),
        sem_ml_s=dma((p.share,)),
        sem_ml_r=dma((p.share,)),
        sem_kv_s=dma((2, p.heads, p.share)),
        sem_kv_r=dma((2, p.heads, p.share)),
        sem_q_s=dma((p.share,)),
        sem_q_r=dma((p.share,)),
        sem_res_s=dma((3, p.heads)),
        sem_res_r=dma((3, p.heads)),
    )
    return items


class Refs:
    pass


INPUTS = (
    "table",
    "rate",
    "res",
    "attn_q",
    "attn_k",
    "attn_v",
    "attn_o",
    "attn_dy",
    "weight",
    "hy_q",
    "hy_k",
    "hy_v",
    "hy_dy",
)
OUTPUTS = ("out_q", "out_k", "out_v", "out_hq", "out_hk", "out_hv")


def column(ref, g):
    x = ref[...]
    lane = lax.broadcasted_iota(jnp.int32, x.shape, 1)
    return jnp.sum(jnp.where(lane == g, x, 0.0), axis=1, keepdims=True)


def kernel(p, names, *refs):
    r = Refs()
    for name, ref in zip(names, refs, strict=True):
        setattr(r, name, ref)
    me = lax.axis_index("ctx").astype(jnp.int32)
    at = lax.axis_index("tp").astype(jnp.int32)
    count, heads, share, tok, half = p.count, p.heads, p.share, p.tok, p.half
    head, turn = me // share, me % share

    def remote(src, dst, send, recv, ctx):
        return pltpu.make_async_remote_copy(
            src_ref=src,
            dst_ref=dst,
            send_sem=send,
            recv_sem=recv,
            device_id={"ctx": ctx},
            device_id_type=MESH,
        )

    def local(src, dst, sem):
        return pltpu.make_async_copy(src, dst, sem)

    def cols(h):
        return rows_at(h, HD)

    def pair_at(i):
        return pl.ds(2 * i, 2)

    barrier = pltpu.get_barrier_semaphore()
    for d in range(1, count):
        pl.semaphore_signal(
            barrier, inc=1, device_id={"ctx": (me + d) % count}, device_id_type=MESH
        )
    for d in range(1, p.parts):
        pl.semaphore_signal(
            barrier, inc=1, device_id={"tp": (at + d) % p.parts}, device_id_type=MESH
        )
    pl.semaphore_wait(barrier, count + p.parts - 2)

    def dy_copy(d, n):
        rows = pl.ds(n * p.piece, p.piece)
        return pltpu.make_async_remote_copy(
            src_ref=r.attn_dy.at[rows, :],
            dst_ref=r.dy_got.at[d - 1, rows, :],
            send_sem=r.sem_dy_s.at[d - 1, n],
            recv_sem=r.sem_dy_r.at[d - 1, n],
            device_id={"tp": (at + d) % p.parts},
            device_id_type=MESH,
        )

    for n in range(p.chunks):
        for d in range(1, p.parts):
            dy_copy(d, n).start()

    def part_cols(d):
        return rows_at((at - d + p.parts) % p.parts, p.width)

    hy_src = (r.hy_q, r.hy_k, r.hy_v, r.hy_dy)
    fetch_hy = [local(hy_src[i], r.hy_in.at[i], r.sem_local.at[i]) for i in range(4)]
    fetch_dy = local(r.attn_dy, r.dy_own, r.sem_local.at[4])
    fetch_w = local(r.weight.at[:, part_cols(0)], r.w_own, r.sem_local.at[5])
    fetch_o = local(r.attn_o, r.o_buf, r.sem_local.at[6])
    sources = (r.attn_k, r.attn_q, r.attn_v)
    alls = (r.k_all, r.q_all, r.v_all)
    seqs = (r.k_seq, r.q_seq, r.v_seq)
    own_slot = pair_at(turn * heads + head)
    fetch_own = [
        local(sources[i].at[:, :, cols(head)], alls[i].at[own_slot], r.sem_local.at[7 + i])
        for i in range(3)
    ]
    for c in fetch_hy:
        c.start()
    fetch_dy.start()
    fetch_w.start()

    def in_copy(i, d, arriving):
        to = (head + d) % heads
        source = (head - d + heads) % heads if arriving else head
        slot = pair_at(turn * heads + source)
        return remote(
            sources[i].at[:, :, cols(to)],
            alls[i].at[slot],
            r.sem_in_s.at[i, d],
            r.sem_in_r.at[i, d],
            to * share + turn,
        )

    for i in range(3):
        loop(1, heads, lambda d, i=i: in_copy(i, d, False).start())
    for c in fetch_own:
        c.start()
    fetch_o.start()
    fetch_rest = []
    for d in range(1, p.parts):
        c = local(r.weight.at[:, part_cols(d)], r.w_rest.at[d - 1], r.sem_rest.at[d - 1])
        fetch_rest.append(c)

    for c in fetch_hy:
        c.wait()
    lane_shape = (p.modes, tok)
    lag = lax.broadcasted_iota(jnp.int32, lane_shape, 1).astype(F32)

    def hy_block(i, g):
        return r.hy_in[i, :, rows_at(g, p.size)].astype(F32)

    def twice(x):
        return jnp.concatenate(split(x), axis=1)

    def state_of(decay, prod):
        both = dot_nn(jnp.concatenate(split(decay), axis=0), twice(prod))
        both = both[: p.modes] + both[p.modes :]
        return both[:, : p.size] + both[:, p.size :]

    def one_state(g):
        rate = column(r.rate, g)
        tail = jnp.exp(-rate * (tok - 1 - lag))
        first = jnp.exp(-rate * lag)
        lines = rows_at(g, p.modes)
        r.st_own[0, lines, :] = state_of(tail, hy_block(1, g) * hy_block(2, g)).astype(BF16)
        r.st_own[1, lines, :] = state_of(first, hy_block(0, g) * hy_block(3, g)).astype(BF16)

    loop(0, p.groups, one_state)

    near, far = p.near, p.far
    my_near, my_far = me % near, me // near

    def near_copy(d, arriving):
        source = (my_near - d + near) % near if arriving else my_near
        return remote(
            r.st_own,
            r.st_got.at[source],
            r.sem_st_s.at[d],
            r.sem_st_r.at[d],
            my_far * near + (my_near + d) % near,
        )

    loop(1, near, lambda d: near_copy(d, False).start())

    fetch_dy.wait()
    fetch_w.wait()
    for c in fetch_rest:
        c.start()

    def own_product(n):
        at_cols = rows_at(n, p.tile)
        r.g_part[:, at_cols] = dot_nt(r.dy_own[...], r.w_own[at_cols, :])

    loop(0, p.feat // p.tile, own_product)

    loop(1, near, lambda d: near_copy(d, True).wait_recv())
    r.st_got[my_near] = r.st_own[...]

    def decay(rate, steps, good):
        power = jnp.exp(-rate * (tok * jnp.maximum(steps, 0)).astype(F32))
        return jnp.where(good, power, 0.0)

    def near_sum(g):
        rate = column(r.rate, g)
        lines = rows_at(g, p.modes)
        zero = jnp.zeros((p.modes, p.size), F32)
        total, back, fin, fin_back = zero, zero, zero, zero
        for other in range(near):
            ahead = r.st_got[other, 0, lines, :].astype(F32)
            behind = r.st_got[other, 1, lines, :].astype(F32)
            total = total + decay(rate, jnp.int32(near - 1 - other), True) * ahead
            back = back + decay(rate, jnp.int32(other), True) * behind
            gap = my_near - 1 - other
            fin = fin + decay(rate, gap, gap >= 0) * ahead
            gap = other - 1 - my_near
            fin_back = fin_back + decay(rate, gap, gap >= 0) * behind
        r.st_far[0, lines, :] = total.astype(BF16)
        r.st_far[1, lines, :] = back.astype(BF16)
        r.st_fin[0, lines, :] = fin
        r.st_fin[1, lines, :] = fin_back

    loop(0, p.groups, near_sum)

    def far_copy(d):
        to = (my_far + d) % far
        return remote(
            r.st_far.at[(my_far + d) // far],
            r.far_got.at[d - 1],
            r.sem_far_s.at[d],
            r.sem_far_r.at[d],
            to * near + my_near,
        )

    loop(1, far, lambda d: far_copy(d).start())

    def hand_on(ref, i, s, arriving, sems):
        source = (turn - s + share) % share if arriving else turn
        part = pl.ds(source * heads * 2, heads * 2)
        return remote(
            ref.at[part],
            ref.at[part],
            sems[0].at[i, s],
            sems[1].at[i, s],
            head * share + (turn + s) % share,
        )

    fw = (r.sem_fw_s, r.sem_fw_r)

    def arrive(i):
        loop(1, heads, lambda d: in_copy(i, d, True).wait_recv())
        fetch_own[i].wait()
        for s in range(1, share):
            hand_on(alls[i], i, s, False, fw).start()

    def in_order(source, target):
        def one(place):
            target[rows_at(place, half), :] = source[r.table[0, place]]

        loop(0, 2 * count, one)

    def settle(i):
        for s in range(1, share):
            hand_on(alls[i], i, s, True, fw).wait_recv()
        in_order(alls[i], seqs[i])

    arrive(0)
    arrive(1)
    settle(0)
    settle(1)

    def g_place(n, source):
        slot, start = divmod(n * p.piece, half)
        return 2 * (turn * heads + source) + slot, pl.ds(start, p.piece)

    def g_copy(n, d, arriving):
        to = (head + d) % heads
        source = (head - d + heads) % heads if arriving else head
        rows = pl.ds(n * p.piece, p.piece)
        slot, inner = g_place(n, source)
        return remote(
            r.g_low.at[rows, cols(to)],
            r.g_all.at[slot, inner, :],
            r.sem_g_s.at[n, d],
            r.sem_g_r.at[n, d],
            to * share + turn,
        )

    def g_chunk(n):
        for d in range(1, p.parts):
            dy_copy(d, n).wait_recv()
        rows = pl.ds(n * p.piece, p.piece)

        def tile(c):
            at_cols = rows_at(c, p.tile)
            total = r.g_part[rows, at_cols]
            for d in range(1, p.parts):
                total = total + dot_nt(r.dy_got[d - 1, rows, :], r.w_rest[d - 1, at_cols, :])
            r.g_low[rows, at_cols] = total.astype(BF16)

        loop(0, p.feat // p.tile, tile)
        loop(1, heads, lambda d: g_copy(n, d, False).start())
        slot, inner = g_place(n, head)
        r.g_all[slot, inner, :] = r.g_low[rows, cols(head)]

    def g_arrive(n):
        loop(1, heads, lambda d: g_copy(n, d, True).wait_recv())

    for c in fetch_rest:
        c.wait()
    g_chunk(0)
    g_chunk(1)

    square = (tok, tok)
    row_id = lax.broadcasted_iota(jnp.int32, (8, tok), 0)
    empty = jnp.where(row_id == 0, NEG_LARGE, 0.0)

    def clear(n):
        r.ml[n] = empty

    loop(0, heads * count, clear)

    def turn_keys(n):
        mine = p.own(n, turn)
        r.k_turn[n] = r.k_seq[rows_at(mine, tok), :].astype(F32).T.astype(BF16)

    loop(0, heads, turn_keys)

    def spread(n):
        mine = p.own(n, turn)
        first = p.offset(n, turn)
        keys = rows_at(mine, tok)

        def one(i, masked=False):
            s = dot_nt(r.k_seq[keys, :], r.q_seq[rows_at(i, tok), :])
            if masked:
                key_id = lax.broadcasted_iota(jnp.int32, square, 0)
                query_id = lax.broadcasted_iota(jnp.int32, square, 1)
                s = jnp.where(key_id <= query_id, s, NEG_LARGE)
            peak = jnp.max(s, axis=0, keepdims=True)
            e = jnp.exp2((s - peak) * LN2_SCALE)
            r.cache[first + i - mine] = e.astype(BF16)
            r.ml[n * count + i, 0:1, :] = peak
            r.ml[n * count + i, 1:2, :] = jnp.sum(e, axis=0, keepdims=True)

        one(mine, True)
        loop(mine + 1, count, one)

    loop(0, heads, spread)

    def combine(i):
        peaks = [r.ml[n * count + i, 0:1, :] for n in range(heads)]
        peak = functools.reduce(jnp.maximum, peaks)
        total = 0.0
        for n in range(heads):
            weight = jnp.exp2((peaks[n] - peak) * LN2_SCALE)
            total = total + weight * r.ml[n * count + i, 1:2, :]
        r.ml_own[i, 0:1, :] = peak
        r.ml_own[i, 1:2, :] = total

    def clear_own(i):
        r.ml_own[i] = empty

    loop(0, count, clear_own)
    loop(0, count, combine)

    def ml_copy(s):
        return remote(
            r.ml_own,
            r.ml_got.at[s - 1],
            r.sem_ml_s.at[s],
            r.sem_ml_r.at[s],
            head * share + (turn + s) % share,
        )

    for s in range(1, share):
        ml_copy(s).start()
    arrive(2)
    g_chunk(2)
    for s in range(1, share):
        ml_copy(s).wait_recv()
        ml_copy(s).wait_send()

    def join(i):
        peaks = [r.ml_own[i, 0:1, :]] + [r.ml_got[s, i, 0:1, :] for s in range(share - 1)]
        peak = functools.reduce(jnp.maximum, peaks)
        total = jnp.exp2((peaks[0] - peak) * LN2_SCALE) * r.ml_own[i, 1:2, :]
        for s in range(share - 1):
            weight = jnp.exp2((peaks[s + 1] - peak) * LN2_SCALE)
            total = total + weight * r.ml_got[s, i, 1:2, :]
        r.ml_own[i, 0:1, :] = peak
        r.ml_own[i, 1:2, :] = 1.0 / total

    loop(0, count, join)

    def normal(n):
        mine = p.own(n, turn)
        first = p.offset(n, turn)

        def one(i):
            weight = jnp.exp2((r.ml[n * count + i, 0:1, :] - r.ml_own[i, 0:1, :]) * LN2_SCALE)
            weight = weight * r.ml_own[i, 1:2, :]
            e = r.cache[first + i - mine].astype(F32)
            r.cache[first + i - mine] = (e * weight).astype(BF16)

        loop(mine, count, one)

    loop(0, heads, normal)
    settle(2)

    loop(1, far, lambda d: far_copy(d).wait_recv())

    def far_sum(g):
        rate = column(r.rate, g)
        lines = rows_at(g, p.modes)
        ahead = jnp.zeros((p.modes, p.size), F32)
        behind = ahead
        for d in range(1, far):
            got = r.far_got[d - 1, lines, :].astype(F32)
            source = (my_far - d + far) % far
            gap = (my_far - 1 - source) * near + my_near
            ahead = ahead + decay(rate, gap, source < my_far) * got
            gap = (source - 1 - my_far) * near + near - 1 - my_near
            behind = behind + decay(rate, gap, source > my_far) * got
        r.st_fin[0, lines, :] += ahead
        r.st_fin[1, lines, :] += behind

    loop(0, p.groups, far_sum)

    gf = (r.sem_gf_s, r.sem_gf_r)

    def g_hand(n, s, arriving):
        source = (turn - s + share) % share if arriving else turn
        part = pl.ds(source * heads * 2, heads * 2)
        return remote(
            r.g_all.at[part],
            r.g_all.at[part],
            gf[0].at[n, s],
            gf[1].at[n, s],
            head * share + (turn + s) % share,
        )

    for n in range(3, p.chunks):
        g_chunk(n)
    fetch_o.wait()
    ones = jnp.ones((8, HD), BF16)

    def delta_of(h):
        prod = r.g_low[:, cols(h)].astype(F32) * r.o_buf[:, cols(h)].astype(F32)
        high, low = split(prod)
        value = dot_nt(ones, high) + dot_nt(ones, low)
        r.delta_out[h, 0] = value[:, :half]
        r.delta_out[h, 1] = value[:, half:]

    loop(0, heads, delta_of)

    def delta_copy(d, arriving):
        to = (head + d) % heads
        source = (head - d + heads) % heads if arriving else head
        return remote(
            r.delta_out.at[to],
            r.delta_all.at[pl.ds((turn * heads + source) * 2, 2)],
            r.sem_d_s.at[d],
            r.sem_d_r.at[d],
            to * share + turn,
        )

    loop(1, heads, lambda d: delta_copy(d, False).start())
    r.delta_all[pl.ds((turn * heads + head) * 2, 2)] = r.delta_out[head]

    def delta_hand(s, arriving):
        source = (turn - s + share) % share if arriving else turn
        part = pl.ds(source * heads * 2, heads * 2)
        return remote(
            r.delta_all.at[part],
            r.delta_all.at[part],
            r.sem_df_s.at[s],
            r.sem_df_r.at[s],
            head * share + (turn + s) % share,
        )

    for n in range(p.chunks):
        g_arrive(n)
    for s in range(1, share):
        g_hand(0, s, False).start()
    loop(1, heads, lambda d: delta_copy(d, True).wait_recv())
    for s in range(1, share):
        delta_hand(s, False).start()
    for s in range(1, share):
        g_hand(0, s, True).wait_recv()
        delta_hand(s, True).wait_recv()
    in_order(r.g_all, r.g_seq)

    def order_delta(place):
        r.delta_seq[place] = r.delta_all[r.table[0, place]]

    loop(0, 2 * count, order_delta)

    def column_pass(kind, other, target, factor):
        def one(n):
            mine = p.own(n, turn)
            first = p.offset(n, turn)

            def add(i, acc):
                return acc + dot_nn(r.cache[first + i - mine], other[rows_at(i, tok), :])

            acc = lax.fori_loop(mine, count, add, jnp.zeros((tok, HD), F32))
            value = (acc * factor).astype(BF16)
            target[2 * mine] = value[:half]
            target[2 * mine + 1] = value[half:]
            for s in range(1, share):
                kv_copy(kind, n, s, target, False).start()

        loop(0, heads, one)

    def kv_copy(kind, n, s, target, arriving):
        source = (turn - s + share) % share if arriving else turn
        rows = pair_at(p.own(n, source))
        return remote(
            target.at[rows],
            target.at[rows],
            r.sem_kv_s.at[kind, n, s],
            r.sem_kv_r.at[kind, n, s],
            head * share + (turn + s) % share,
        )

    def kv_arrive(kind, target):
        def one(n):
            for s in range(1, share):
                kv_copy(kind, n, s, target, True).wait_recv()

        loop(0, heads, one)

    outs = (r.out_q, r.out_k, r.out_v)

    def res_copy(kind, d):
        to = (head + d) % heads
        return remote(
            r.send.at[kind, d],
            outs[kind].at[:, :, cols(head)],
            r.sem_res_s.at[kind, d],
            r.sem_res_r.at[kind, d],
            to * share + turn,
        )

    def res_local(kind):
        return local(r.send.at[kind, 0], outs[kind].at[:, :, cols(head)], r.sem_out.at[kind])

    def hand_back(kind, value_of):
        def one(d):
            flat = (turn * heads + (head + d) % heads) * 2
            for b in range(2):
                place = r.table[1, flat + b]
                value = value_of(place, (head + d) % heads, b)
                r.send[kind, d, b] = value

        def both(d):
            one(d)
            res_copy(kind, d).start()

        loop(1, heads, both)
        one(0)
        res_local(kind).start()

    column_pass(0, r.g_seq, r.dv_seq, 1.0)
    kv_arrive(0, r.dv_seq)
    hand_back(2, lambda place, h, b: r.dv_seq[place])

    def row_pass(i):
        g = r.g_seq[rows_at(i, tok), :]
        delta = jnp.concatenate(
            [r.delta_seq[2 * i, 0:1, :], r.delta_seq[2 * i + 1, 0:1, :]], axis=1
        )

        def one(n, acc):
            mine = p.own(n, turn)
            where = p.offset(n, turn) + i - mine
            grad_prob = dot_nt(r.v_seq[rows_at(mine, tok), :], g)
            grad_score = (r.cache[where].astype(F32) * (grad_prob - delta)).astype(BF16)
            r.cache[where] = grad_score
            return acc + dot_nn(r.k_turn[n], grad_score)

        acc = lax.fori_loop(0, p.held(i, turn), one, jnp.zeros((HD, tok), F32))
        value = acc.T * SCALE
        r.dq_seq[2 * i] = value[:half]
        r.dq_seq[2 * i + 1] = value[half:]

    loop(0, count, row_pass)

    def q_copy(s):
        return remote(
            r.dq_out.at[s - 1],
            r.dq_got.at[s - 1],
            r.sem_q_s.at[s],
            r.sem_q_r.at[s],
            head * share + (turn + s) % share,
        )

    for s in range(1, share):

        def pick(f, s=s):
            place = r.table[1, (turn + s) % share * heads * 2 + f]
            r.dq_out[s - 1, f] = r.dq_seq[place]

        loop(0, 2 * heads, pick)
        q_copy(s).start()

    column_pass(1, r.q_seq, r.dk_seq, SCALE)
    for s in range(1, share):
        q_copy(s).wait_recv()

    def dq_value(place, h, b):
        value = r.dq_seq[place]
        for s in range(1, share):
            value = value + r.dq_got[s - 1, 2 * h + b]
        return value.astype(BF16)

    hand_back(0, dq_value)
    kv_arrive(1, r.dk_seq)
    hand_back(1, lambda place, h, b: r.dk_seq[place])

    lag_id = lax.broadcasted_iota(jnp.int32, lane_shape, 1)
    turned = jnp.where(lag_id == 0, 0, tok - lag_id).astype(F32)
    tall = (half, tok)
    row = lax.broadcasted_iota(jnp.int32, (half, half), 0)
    col = lax.broadcasted_iota(jnp.int32, (half, half), 1)
    blank = jnp.zeros((half, half), F32)

    def mixed(bands, prod, edge, state):
        high, low = split(bands)
        pair = twice(prod)
        out = dot_nn(high, pair) + dot_nn(low, pair)
        e_high = edge.astype(BF16).astype(F32)
        s_high, s_low = split(state)
        left = jnp.concatenate([e_high, edge - e_high, e_high], axis=0).T.astype(BF16)
        right = jnp.concatenate([s_high, s_high, s_low], axis=0)
        return out[:, : p.size] + out[:, p.size :] + dot_nn(left, right)

    def mix(g):
        rate = jnp.broadcast_to(column(r.rate, g), lane_shape)
        res = jnp.broadcast_to(column(r.res, g), lane_shape)
        taps = jnp.sum(res * jnp.exp(-rate * lag), axis=0, keepdims=True)
        back_taps = jnp.sum(res * jnp.exp(-rate * turned), axis=0, keepdims=True)
        lower = pltpu.roll(jnp.broadcast_to(back_taps, tall), 0, 1, stride=1, stride_axis=0)
        upper = pltpu.roll(jnp.broadcast_to(taps, tall), 0, 1, stride=1, stride_axis=0)
        near_low = jnp.where(col <= row, lower[:, :half], 0.0)
        near_up = jnp.where(col >= row, upper[:, :half], 0.0)
        lower = jnp.concatenate(
            [
                jnp.concatenate([near_low, blank], axis=1),
                jnp.concatenate([lower[:, half:], near_low], axis=1),
            ],
            axis=0,
        )
        upper = jnp.concatenate(
            [
                jnp.concatenate([near_up, upper[:, half:]], axis=1),
                jnp.concatenate([blank, near_up], axis=1),
            ],
            axis=0,
        )
        lines = rows_at(g, p.modes)
        into = res * jnp.exp(-rate * (lag + 1.0))
        back = res * jnp.exp(-rate * (tok - lag))
        k, v, dy = hy_block(1, g), hy_block(2, g), hy_block(3, g)
        conv = mixed(lower, k * v, into, r.st_fin[0, lines, :])
        mid = mixed(upper, hy_block(0, g) * dy, back, r.st_fin[1, lines, :])
        here = rows_at(g, p.size)
        r.hy_out[0, :, here] = (dy * conv).astype(BF16)
        r.hy_out[1, :, here] = (mid * v).astype(BF16)
        r.hy_out[2, :, here] = (mid * k).astype(BF16)

    loop(0, p.groups, mix)
    hy_outs = (r.out_hq, r.out_hk, r.out_hv)
    give = [local(r.hy_out.at[i], hy_outs[i], r.sem_out.at[3 + i]) for i in range(3)]
    for c in give:
        c.start()

    for n in range(p.chunks):
        for d in range(1, p.parts):
            dy_copy(d, n).wait_send()
    loop(1, near, lambda d: near_copy(d, False).wait_send())
    loop(1, far, lambda d: far_copy(d).wait_send())
    for i in range(3):
        loop(1, heads, lambda d, i=i: in_copy(i, d, False).wait_send())
        for s in range(1, share):
            hand_on(alls[i], i, s, False, fw).wait_send()
    for n in range(p.chunks):
        loop(1, heads, lambda d, n=n: g_copy(n, d, False).wait_send())
    loop(1, heads, lambda d: delta_copy(d, False).wait_send())
    for s in range(1, share):
        g_hand(0, s, False).wait_send()
        delta_hand(s, False).wait_send()
        q_copy(s).wait_send()

        def kv_sent(n, s=s):
            kv_copy(0, n, s, r.dv_seq, False).wait_send()
            kv_copy(1, n, s, r.dk_seq, False).wait_send()

        loop(0, heads, kv_sent)
    for kind in range(3):
        loop(1, heads, lambda d, kind=kind: res_copy(kind, d).wait_send())
        loop(1, heads, lambda d, kind=kind: res_copy(kind, d).wait_recv())
        res_local(kind).wait()
    for c in give:
        c.wait()


def body(
    attn_q,
    attn_k,
    attn_v,
    attn_o,
    attn_dy,
    out_weight,
    block_place,
    hyena_q,
    hyena_k,
    hyena_v,
    hyena_dy,
    filter_residue,
    filter_rate,
):
    tok, feat = attn_q.shape
    chan = hyena_q.shape[1]
    modes, groups = filter_rate.shape
    count, parts = lax.axis_size("ctx"), lax.axis_size("tp")
    p = Plan(count, parts, tok, feat, attn_dy.shape[1], chan, modes, groups)
    places = block_place.reshape(p.heads, p.share, 2).transpose(1, 0, 2).reshape(-1)
    slot = jnp.arange(2 * count, dtype=jnp.int32)
    found = jnp.where(places[None, :] == slot[:, None], slot[None, :], 0)
    table = jnp.stack([jnp.sum(found, axis=1), places])
    items = scratch(p)
    names = INPUTS + OUTPUTS + tuple(items)
    hbm = pl.BlockSpec(memory_space=pl.ANY)
    vmem = pl.BlockSpec(memory_space=pltpu.VMEM)
    attn_out = jax.ShapeDtypeStruct((2, p.half, feat), BF16)
    hy_out = jax.ShapeDtypeStruct((tok, chan), BF16)
    outs = pl.pallas_call(
        functools.partial(kernel, p, names),
        in_specs=[pl.BlockSpec(memory_space=pltpu.SMEM), vmem, vmem] + [hbm] * 10,
        out_specs=[hbm] * 6,
        out_shape=[attn_out] * 3 + [hy_out] * 3,
        scratch_shapes=list(items.values()),
        compiler_params=pltpu.CompilerParams(
            collective_id=0, has_side_effects=True, vmem_limit_bytes=63 * 1024 * 1024
        ),
        name="grads",
    )(
        table,
        filter_rate,
        filter_residue,
        attn_q.reshape(2, p.half, feat),
        attn_k.reshape(2, p.half, feat),
        attn_v.reshape(2, p.half, feat),
        attn_o,
        attn_dy,
        out_weight,
        hyena_q,
        hyena_k,
        hyena_v,
        hyena_dy,
    )
    return tuple(x.reshape(tok, feat) for x in outs[:3]) + tuple(outs[3:])


def solution(mesh):
    both = P("ctx", "tp")
    in_specs = (both,) * 5 + (P("tp", None), P()) + (both,) * 4 + (P(None, "tp"),) * 2
    return jax.shard_map(body, mesh=mesh, in_specs=in_specs, out_specs=(both,) * 6, check_vma=False)
```

```python
import functools
import math

import jax
import jax.numpy as jnp
from jax import lax
from jax.experimental import pallas as pl
from jax.experimental.pallas import tpu as pltpu
from jax.sharding import PartitionSpec as P

HD = 128
NEG_LARGE = -1e30
F32 = jnp.float32
BF16 = jnp.bfloat16
MESH = pl.DeviceIdType.MESH
LN2_SCALE = HD ** (-0.5) * math.log2(math.e)
SCALE = HD ** (-0.5)


def dot_nn(a, b):
    return lax.dot_general(a, b, (((1,), (0,)), ((), ())), preferred_element_type=F32)


def dot_nt(a, b):
    return lax.dot_general(a, b, (((1,), (1,)), ((), ())), preferred_element_type=F32)


def split(x):
    high = x.astype(BF16)
    return high, (x - high.astype(F32)).astype(BF16)


def rows_at(block, size):
    return pl.ds(pl.multiple_of(block * size, size), size)


def loop(start, stop, fn):
    def step(i, carry):
        fn(i)
        return carry

    lax.fori_loop(start, stop, step, 0)


def spans(start, stop, fn, carry=0):
    for width in (4, 2, 1):
        turns = (stop - start) // width
        carry = lax.fori_loop(
            0, turns, lambda t, c, s=start, w=width: fn(s + w * t, w, c), carry
        )
        start = start + width * turns
    return carry


class Plan:
    def __init__(self, count, parts, tok, feat, width, chan, modes, groups):
        self.count, self.parts = count, parts
        self.tok, self.feat, self.width = tok, feat, width
        self.chan, self.modes, self.groups = chan, modes, groups
        self.heads = feat // HD
        self.share = count // self.heads
        self.half = tok // 2
        self.near = 4 if count % 4 == 0 else count
        self.far = count // self.near
        self.chunks = 4
        self.piece = tok // self.chunks
        self.tile = min(256, feat)
        self.size = chan // groups
        self.blocks = max(
            sum(count - self.own(n, turn) for n in range(self.heads)) for turn in range(self.share)
        )

    def own(self, n, turn):
        return n * self.share + turn + (n % 2) * (self.share - 1 - 2 * turn)

    def offset(self, n, turn):
        share = self.share
        before = (
            share * (n * (n - 1) // 2) + ((n + 1) // 2) * turn + (n // 2) * (share - 1 - turn)
        )
        return n * self.count - before

    def held(self, i, turn):
        at = i // self.share
        mine = self.own(at, turn) - at * self.share
        return at + (i % self.share - mine + self.share) // self.share


def scratch(p):
    vm = pltpu.VMEM
    total = p.count * p.tok
    low = vm((total, HD), BF16)
    blocked = vm((2 * p.count, p.half, HD), BF16)
    other = max(p.share - 1, 1)
    rest = max(p.parts - 1, 1)
    lines = p.groups * p.modes
    dma = pltpu.SemaphoreType.DMA

    def pair(*shape):
        return [dma(shape), dma(shape)]

    items = dict(
        dy_own=vm((p.tok, p.width), BF16),
        dy_got=vm((rest, p.tok, p.width), BF16),
        w_own=vm((p.feat, p.width), BF16),
        w_rest=vm((rest, p.feat, p.width), BF16),
        g_part=vm((p.tok, p.feat), F32),
        o_buf=vm((p.tok, p.feat), BF16),
        g_low=vm((p.tok, p.feat), BF16),
        table=pltpu.SMEM((2, 2 * p.count), jnp.int32),
        delta_out=vm((2, p.heads, 8, HD), F32),
        delta_all=vm((2 * p.count, 8, HD), F32),
        delta_row=vm((p.count, 8, p.tok), F32),
        q_all=blocked,
        k_all=blocked,
        v_all=blocked,
        g_all=blocked,
        q_seq=low,
        k_seq=low,
        v_seq=low,
        g_seq=low,
        k_turn=vm((p.heads, HD, p.tok), BF16),
        cache=vm((p.blocks, p.tok, p.tok), BF16),
        ml=vm((p.heads * p.count, 8, p.tok), F32),
        ml_own=vm((p.count, 8, p.tok), F32),
        ml_got=vm((other, p.count, 8, p.tok), F32),
        dq_turn=vm((p.count, HD, p.tok), F32),
        dq_seq=vm((2 * p.count, p.half, HD), F32),
        dq_out=vm((other, 2 * p.heads, p.half, HD), F32),
        dq_got=vm((other, 2 * p.heads, p.half, HD), F32),
        dk_seq=blocked,
        dv_seq=blocked,
        send=vm((3, p.heads, 2, p.half, HD), BF16),
        hy_in=vm((4, p.tok, p.chan), BF16),
        hy_out=vm((3, p.tok, p.chan), BF16),
        st_own=vm((2, lines, HD), BF16),
        st_got=vm((p.near, 2, lines, HD), BF16),
        st_far=vm((2, lines, HD), BF16),
        far_got=vm((max(p.far - 1, 1), lines, HD), BF16),
        st_fin=vm((2, lines, HD), F32),
        sem_local=dma((16,)),
        sem_rest=dma((rest,)),
        sem_out=dma((6,)),
        sem_dy_s=dma((rest, p.chunks)),
        sem_dy_r=dma((rest, p.chunks)),
        sem_in_s=dma((3, p.heads)),
        sem_in_r=dma((3, p.heads)),
        sem_fw_s=dma((3, p.share)),
        sem_fw_r=dma((3, p.share)),
        sem_g_s=dma((p.chunks, p.heads)),
        sem_g_r=dma((p.chunks, p.heads)),
        sem_gf_s=dma((p.chunks, p.share)),
        sem_gf_r=dma((p.chunks, p.share)),
        sem_d_s=dma((2, p.heads)),
        sem_d_r=dma((2, p.heads)),
        sem_df_s=dma((2, p.share)),
        sem_df_r=dma((2, p.share)),
        sem_st_s=dma((p.near,)),
        sem_st_r=dma((p.near,)),
        sem_far_s=dma((p.far,)),
        sem_far_r=dma((p.far,)),
        sem_ml_s=dma((p.share,)),
        sem_ml_r=dma((p.share,)),
        sem_kv_s=dma((2, p.heads, p.share)),
        sem_kv_r=dma((2, p.heads, p.share)),
        sem_q_s=dma((p.share,)),
        sem_q_r=dma((p.share,)),
        sem_res_s=dma((3, p.heads)),
        sem_res_r=dma((3, p.heads)),
    )
    return items


class Refs:
    pass


INPUTS = (
    "places",
    "rate",
    "res",
    "attn_q",
    "attn_k",
    "attn_v",
    "attn_o",
    "attn_dy",
    "weight",
    "hy_q",
    "hy_k",
    "hy_v",
    "hy_dy",
)
OUTPUTS = ("out_q", "out_k", "out_v", "out_hq", "out_hk", "out_hv")


def column(ref, g):
    x = ref[...]
    lane = lax.broadcasted_iota(jnp.int32, x.shape, 1)
    return jnp.sum(jnp.where(lane == g, x, 0.0), axis=1, keepdims=True)


def kernel(p, names, *refs):
    r = Refs()
    for name, ref in zip(names, refs, strict=True):
        setattr(r, name, ref)
    me = lax.axis_index("ctx").astype(jnp.int32)
    at = lax.axis_index("tp").astype(jnp.int32)
    count, heads, share, tok, half = p.count, p.heads, p.share, p.tok, p.half
    head, turn = me // share, me % share

    def remote(src, dst, send, recv, ctx):
        return pltpu.make_async_remote_copy(
            src_ref=src,
            dst_ref=dst,
            send_sem=send,
            recv_sem=recv,
            device_id={"ctx": ctx},
            device_id_type=MESH,
        )

    def local(src, dst, sem):
        return pltpu.make_async_copy(src, dst, sem)

    def cols(h):
        return rows_at(h, HD)

    def pair_at(i):
        return pl.ds(2 * i, 2)

    barrier = pltpu.get_barrier_semaphore()
    for d in range(1, count):
        pl.semaphore_signal(
            barrier, inc=1, device_id={"ctx": (me + d) % count}, device_id_type=MESH
        )
    for d in range(1, p.parts):
        pl.semaphore_signal(
            barrier, inc=1, device_id={"tp": (at + d) % p.parts}, device_id_type=MESH
        )
    pl.semaphore_wait(barrier, count + p.parts - 2)

    def dy_copy(d, n):
        rows = pl.ds(n * p.piece, p.piece)
        return pltpu.make_async_remote_copy(
            src_ref=r.attn_dy.at[rows, :],
            dst_ref=r.dy_got.at[d - 1, rows, :],
            send_sem=r.sem_dy_s.at[d - 1, n],
            recv_sem=r.sem_dy_r.at[d - 1, n],
            device_id={"tp": (at + d) % p.parts},
            device_id_type=MESH,
        )

    for n in range(p.chunks):
        for d in range(1, p.parts):
            dy_copy(d, n).start()

    def part_cols(d):
        return rows_at((at - d + p.parts) % p.parts, p.width)

    hy_src = (r.hy_q, r.hy_k, r.hy_v, r.hy_dy)
    fetch_hy = [local(hy_src[i], r.hy_in.at[i], r.sem_local.at[i]) for i in range(4)]
    fetch_dy = local(r.attn_dy, r.dy_own, r.sem_local.at[4])
    fetch_w = local(r.weight.at[:, part_cols(0)], r.w_own, r.sem_local.at[5])
    fetch_o = local(r.attn_o, r.o_buf, r.sem_local.at[6])
    sources = (r.attn_k, r.attn_q, r.attn_v)
    alls = (r.k_all, r.q_all, r.v_all)
    seqs = (r.k_seq, r.q_seq, r.v_seq)
    own_slot = pair_at(turn * heads + head)
    fetch_own = [
        local(sources[i].at[:, :, cols(head)], alls[i].at[own_slot], r.sem_local.at[7 + i])
        for i in range(3)
    ]
    for c in fetch_hy:
        c.start()
    fetch_dy.start()
    fetch_w.start()

    def in_copy(i, d, arriving):
        to = (head + d) % heads
        source = (head - d + heads) % heads if arriving else head
        slot = pair_at(turn * heads + source)
        return remote(
            sources[i].at[:, :, cols(to)],
            alls[i].at[slot],
            r.sem_in_s.at[i, d],
            r.sem_in_r.at[i, d],
            to * share + turn,
        )

    for i in range(2):
        loop(1, heads, lambda d, i=i: in_copy(i, d, False).start())
    for c in fetch_own:
        c.start()
    fetch_o.start()
    fetch_rest = []
    for d in range(1, p.parts):
        c = local(r.weight.at[:, part_cols(d)], r.w_rest.at[d - 1], r.sem_rest.at[d - 1])
        fetch_rest.append(c)

    for c in fetch_hy:
        c.wait()
    lane_shape = (p.modes, tok)
    lag = lax.broadcasted_iota(jnp.int32, lane_shape, 1).astype(F32)

    def hy_block(i, g):
        return r.hy_in[i, :, rows_at(g, p.size)].astype(F32)

    def twice(x):
        return jnp.concatenate(split(x), axis=1)

    def state_of(decay, prod):
        both = dot_nn(jnp.concatenate(split(decay), axis=0), twice(prod))
        both = both[: p.modes] + both[p.modes :]
        return both[:, : p.size] + both[:, p.size :]

    def one_state(g):
        rate = column(r.rate, g)
        tail = jnp.exp(-rate * (tok - 1 - lag))
        first = jnp.exp(-rate * lag)
        lines = rows_at(g, p.modes)
        r.st_own[0, lines, :] = state_of(tail, hy_block(1, g) * hy_block(2, g)).astype(BF16)
        r.st_own[1, lines, :] = state_of(first, hy_block(0, g) * hy_block(3, g)).astype(BF16)

    loop(0, p.groups, one_state)

    near, far = p.near, p.far
    my_near, my_far = me % near, me // near

    def near_copy(d, arriving):
        source = (my_near - d + near) % near if arriving else my_near
        return remote(
            r.st_own,
            r.st_got.at[source],
            r.sem_st_s.at[d],
            r.sem_st_r.at[d],
            my_far * near + (my_near + d) % near,
        )

    loop(1, near, lambda d: near_copy(d, False).start())

    fetch_dy.wait()
    fetch_w.wait()
    for c in fetch_rest:
        c.start()

    def own_product(n):
        at_cols = rows_at(n, p.tile)
        r.g_part[:, at_cols] = dot_nt(r.dy_own[...], r.w_own[at_cols, :])

    loop(0, p.feat // p.tile, own_product)

    loop(1, near, lambda d: near_copy(d, True).wait_recv())
    r.st_got[my_near] = r.st_own[...]

    def decay(rate, steps, good):
        power = jnp.exp(-rate * (tok * jnp.maximum(steps, 0)).astype(F32))
        return jnp.where(good, power, 0.0)

    def near_sum(g):
        rate = column(r.rate, g)
        lines = rows_at(g, p.modes)
        zero = jnp.zeros((p.modes, p.size), F32)
        total, back, fin, fin_back = zero, zero, zero, zero
        for other in range(near):
            ahead = r.st_got[other, 0, lines, :].astype(F32)
            behind = r.st_got[other, 1, lines, :].astype(F32)
            total = total + decay(rate, jnp.int32(near - 1 - other), True) * ahead
            back = back + decay(rate, jnp.int32(other), True) * behind
            gap = my_near - 1 - other
            fin = fin + decay(rate, gap, gap >= 0) * ahead
            gap = other - 1 - my_near
            fin_back = fin_back + decay(rate, gap, gap >= 0) * behind
        r.st_far[0, lines, :] = total.astype(BF16)
        r.st_far[1, lines, :] = back.astype(BF16)
        r.st_fin[0, lines, :] = fin
        r.st_fin[1, lines, :] = fin_back

    loop(0, p.groups, near_sum)

    def far_copy(d):
        to = (my_far + d) % far
        return remote(
            r.st_far.at[(my_far + d) // far],
            r.far_got.at[d - 1],
            r.sem_far_s.at[d],
            r.sem_far_r.at[d],
            to * near + my_near,
        )

    loop(1, far, lambda d: far_copy(d).start())

    def place_of(flat):
        source, h = flat // (2 * heads), flat // 2 % heads
        return r.places[(h * share + source) * 2 + flat % 2]

    def find(place):
        slot = jnp.int32(0)
        for stored in range(2 * count):
            c, b = divmod(stored, 2)
            flat = c % share * heads + c // share
            slot = jnp.where(r.places[stored] == place, 2 * flat + b, slot)
        r.table[0, place] = slot
        r.table[1, place] = slot % 2 * count + slot // 2

    loop(0, 2 * count, find)

    def clear_queries(i):
        r.dq_turn[i] = jnp.zeros((HD, tok), F32)

    loop(0, count, clear_queries)
    row_id = lax.broadcasted_iota(jnp.int32, (8, tok), 0)
    empty = jnp.where(row_id == 0, NEG_LARGE, 0.0)

    def clear(n):
        r.ml[n] = empty

    loop(0, heads * count, clear)

    def hand_on(ref, i, s, arriving, sems):
        source = (turn - s + share) % share if arriving else turn
        part = pl.ds(source * heads * 2, heads * 2)
        return remote(
            ref.at[part],
            ref.at[part],
            sems[0].at[i, s],
            sems[1].at[i, s],
            head * share + (turn + s) % share,
        )

    fw = (r.sem_fw_s, r.sem_fw_r)

    def arrive(i):
        loop(1, heads, lambda d: in_copy(i, d, True).wait_recv())
        fetch_own[i].wait()
        for s in range(1, share):
            hand_on(alls[i], i, s, False, fw).start()

    def in_order(source, target, row):
        def one(place):
            target[rows_at(place, half), :] = source[r.table[row, place]]

        loop(0, 2 * count, one)

    def settle(i):
        for s in range(1, share):
            hand_on(alls[i], i, s, True, fw).wait_recv()
        in_order(alls[i], seqs[i], 0)

    def g_place(n, source):
        slot, start = divmod(n * p.piece, half)
        return slot * count + turn * heads + source, pl.ds(start, p.piece)

    def g_copy(n, d, arriving):
        to = (head + d) % heads
        source = (head - d + heads) % heads if arriving else head
        rows = pl.ds(n * p.piece, p.piece)
        slot, inner = g_place(n, source)
        return remote(
            r.g_low.at[rows, cols(to)],
            r.g_all.at[slot, inner, :],
            r.sem_g_s.at[n, d],
            r.sem_g_r.at[n, d],
            to * share + turn,
        )

    def g_chunk(n):
        for d in range(1, p.parts):
            dy_copy(d, n).wait_recv()
        rows = pl.ds(n * p.piece, p.piece)

        def tile(c):
            at_cols = rows_at(c, p.tile)
            total = dot_nt(r.w_rest[0, at_cols, :], r.dy_got[0, rows, :])
            for d in range(2, p.parts):
                total = total + dot_nt(r.w_rest[d - 1, at_cols, :], r.dy_got[d - 1, rows, :])
            r.g_low[rows, at_cols] = (r.g_part[rows, at_cols] + total.T).astype(BF16)

        loop(0, p.feat // p.tile, tile)
        loop(1, heads, lambda d: g_copy(n, d, False).start())
        slot, inner = g_place(n, head)
        r.g_all[slot, inner, :] = r.g_low[rows, cols(head)]

    def g_hand(n, s, arriving):
        source = (turn - s + share) % share if arriving else turn
        slot, start = divmod(n * p.piece, half)
        part = r.g_all.at[
            pl.ds(slot * count + source * heads, heads), pl.ds(start, p.piece), :
        ]
        return remote(
            part,
            part,
            r.sem_gf_s.at[n, s],
            r.sem_gf_r.at[n, s],
            head * share + (turn + s) % share,
        )

    def g_arrive(n):
        loop(1, heads, lambda d: g_copy(n, d, True).wait_recv())
        for s in range(1, share):
            g_hand(n, s, False).start()

    ones = jnp.ones((8, HD), BF16)

    def delta_copy(b, d, arriving):
        to = (head + d) % heads
        source = (head - d + heads) % heads if arriving else head
        return remote(
            r.delta_out.at[b, to],
            r.delta_all.at[b * count + turn * heads + source],
            r.sem_d_s.at[b, d],
            r.sem_d_r.at[b, d],
            to * share + turn,
        )

    def delta_half(b):
        rows = pl.ds(b * half, half)

        def one(h):
            prod = r.g_low[rows, cols(h)].astype(F32) * r.o_buf[rows, cols(h)].astype(F32)
            high, low = split(prod)
            r.delta_out[b, h] = dot_nt(ones, high) + dot_nt(ones, low)

        loop(0, heads, one)
        loop(1, heads, lambda d: delta_copy(b, d, False).start())
        r.delta_all[b * count + turn * heads + head] = r.delta_out[b, head]

    def delta_hand(b, s, arriving):
        source = (turn - s + share) % share if arriving else turn
        part = r.delta_all.at[pl.ds(b * count + source * heads, heads)]
        return remote(
            part,
            part,
            r.sem_df_s.at[b, s],
            r.sem_df_r.at[b, s],
            head * share + (turn + s) % share,
        )

    def delta_arrive(b):
        loop(1, heads, lambda d: delta_copy(b, d, True).wait_recv())
        for s in range(1, share):
            delta_hand(b, s, False).start()

    square = (tok, tok)

    def turn_keys(n):
        mine = p.own(n, turn)
        r.k_turn[n] = r.k_seq[rows_at(mine, tok), :].astype(F32).T.astype(BF16)

    def spread(n):
        mine = p.own(n, turn)
        first = p.offset(n, turn)
        keys = rows_at(mine, tok)

        def one(i, masked=False):
            s = dot_nt(r.k_seq[keys, :], r.q_seq[rows_at(i, tok), :])
            if masked:
                key_id = lax.broadcasted_iota(jnp.int32, square, 0)
                query_id = lax.broadcasted_iota(jnp.int32, square, 1)
                s = jnp.where(key_id <= query_id, s, NEG_LARGE)
            peak = jnp.max(s, axis=0, keepdims=True)
            e = jnp.exp2((s - peak) * LN2_SCALE)
            r.cache[first + i - mine] = e.astype(BF16)
            r.ml[n * count + i, 0:1, :] = peak
            r.ml[n * count + i, 1:2, :] = jnp.sum(e, axis=0, keepdims=True)

        def some(i, width, carry):
            for u in range(width):
                one(i + u)
            return carry

        one(mine, True)
        spans(mine + 1, count, some)

    def combine(i):
        peaks = [r.ml[n * count + i, 0:1, :] for n in range(heads)]
        peak = functools.reduce(jnp.maximum, peaks)
        total = 0.0
        for n in range(heads):
            weight = jnp.exp2((peaks[n] - peak) * LN2_SCALE)
            total = total + weight * r.ml[n * count + i, 1:2, :]
        r.ml_own[i] = empty
        r.ml_own[i, 0:1, :] = peak
        r.ml_own[i, 1:2, :] = total

    def ml_copy(s):
        return remote(
            r.ml_own,
            r.ml_got.at[s - 1],
            r.sem_ml_s.at[s],
            r.sem_ml_r.at[s],
            head * share + (turn + s) % share,
        )

    def join(i):
        peaks = [r.ml_own[i, 0:1, :]] + [r.ml_got[s, i, 0:1, :] for s in range(share - 1)]
        peak = functools.reduce(jnp.maximum, peaks)
        total = jnp.exp2((peaks[0] - peak) * LN2_SCALE) * r.ml_own[i, 1:2, :]
        for s in range(share - 1):
            weight = jnp.exp2((peaks[s + 1] - peak) * LN2_SCALE)
            total = total + weight * r.ml_got[s, i, 1:2, :]
        r.ml_own[i, 0:1, :] = peak
        r.ml_own[i, 1:2, :] = 1.0 / total

    def normal(n):
        mine = p.own(n, turn)
        first = p.offset(n, turn)

        def one(i):
            weight = jnp.exp2((r.ml[n * count + i, 0:1, :] - r.ml_own[i, 0:1, :]) * LN2_SCALE)
            weight = weight * r.ml_own[i, 1:2, :]
            e = r.cache[first + i - mine].astype(F32)
            r.cache[first + i - mine] = (e * weight).astype(BF16)

        loop(mine, count, one)

    def far_sum(g):
        rate = column(r.rate, g)
        lines = rows_at(g, p.modes)
        ahead = jnp.zeros((p.modes, p.size), F32)
        behind = ahead
        for d in range(1, far):
            got = r.far_got[d - 1, lines, :].astype(F32)
            source = (my_far - d + far) % far
            gap = (my_far - 1 - source) * near + my_near
            ahead = ahead + decay(rate, gap, source < my_far) * got
            gap = (source - 1 - my_far) * near + near - 1 - my_near
            behind = behind + decay(rate, gap, source > my_far) * got
        r.st_fin[0, lines, :] += ahead
        r.st_fin[1, lines, :] += behind

    lag_id = lax.broadcasted_iota(jnp.int32, lane_shape, 1)
    turned = jnp.where(lag_id == 0, 0, tok - lag_id).astype(F32)
    tall = (half, tok)
    row = lax.broadcasted_iota(jnp.int32, (half, half), 0)
    col = lax.broadcasted_iota(jnp.int32, (half, half), 1)
    blank = jnp.zeros((half, half), F32)

    def mixed(bands, prod, edge, state):
        high, low = split(bands)
        pair = twice(prod)
        out = dot_nn(high, pair) + dot_nn(low, pair)
        e_high = edge.astype(BF16).astype(F32)
        s_high, s_low = split(state)
        left = jnp.concatenate([e_high, edge - e_high, e_high], axis=0).T.astype(BF16)
        right = jnp.concatenate([s_high, s_high, s_low], axis=0)
        return out[:, : p.size] + out[:, p.size :] + dot_nn(left, right)

    def mix(g):
        rate = jnp.broadcast_to(column(r.rate, g), lane_shape)
        res = jnp.broadcast_to(column(r.res, g), lane_shape)
        taps = jnp.sum(res * jnp.exp(-rate * lag), axis=0, keepdims=True)
        back_taps = jnp.sum(res * jnp.exp(-rate * turned), axis=0, keepdims=True)
        lower = pltpu.roll(jnp.broadcast_to(back_taps, tall), 0, 1, stride=1, stride_axis=0)
        upper = pltpu.roll(jnp.broadcast_to(taps, tall), 0, 1, stride=1, stride_axis=0)
        near_low = jnp.where(col <= row, lower[:, :half], 0.0)
        near_up = jnp.where(col >= row, upper[:, :half], 0.0)
        lower = jnp.concatenate(
            [
                jnp.concatenate([near_low, blank], axis=1),
                jnp.concatenate([lower[:, half:], near_low], axis=1),
            ],
            axis=0,
        )
        upper = jnp.concatenate(
            [
                jnp.concatenate([near_up, upper[:, half:]], axis=1),
                jnp.concatenate([blank, near_up], axis=1),
            ],
            axis=0,
        )
        lines = rows_at(g, p.modes)
        into = res * jnp.exp(-rate * (lag + 1.0))
        back = res * jnp.exp(-rate * (tok - lag))
        k, v, dy = hy_block(1, g), hy_block(2, g), hy_block(3, g)
        conv = mixed(lower, k * v, into, r.st_fin[0, lines, :])
        mid = mixed(upper, hy_block(0, g) * dy, back, r.st_fin[1, lines, :])
        here = rows_at(g, p.size)
        r.hy_out[0, :, here] = (dy * conv).astype(BF16)
        r.hy_out[1, :, here] = (mid * v).astype(BF16)
        r.hy_out[2, :, here] = (mid * k).astype(BF16)

    hy_outs = (r.out_hq, r.out_hk, r.out_hv)
    give = [local(r.hy_out.at[i], hy_outs[i], r.sem_out.at[3 + i]) for i in range(3)]

    for c in fetch_rest:
        c.wait()
    g_chunk(0)
    arrive(0)
    arrive(1)
    loop(1, heads, lambda d: in_copy(2, d, False).start())
    settle(0)
    settle(1)
    g_arrive(0)
    loop(0, heads, turn_keys)
    loop(0, heads, spread)
    loop(0, count, combine)
    for s in range(1, share):
        ml_copy(s).start()
    g_chunk(1)
    fetch_o.wait()
    delta_half(0)
    for s in range(1, share):
        ml_copy(s).wait_recv()
        ml_copy(s).wait_send()
    loop(0, count, join)
    loop(0, heads, normal)
    g_arrive(1)
    delta_arrive(0)
    loop(1, far, lambda d: far_copy(d).wait_recv())
    loop(0, p.groups, far_sum)
    g_chunk(2)
    loop(0, p.groups, mix)
    for c in give:
        c.start()
    arrive(2)
    g_arrive(2)
    settle(2)
    g_chunk(3)
    delta_half(1)
    g_arrive(3)
    delta_arrive(1)
    for s in range(1, share):
        for n in range(p.chunks):
            g_hand(n, s, True).wait_recv()
        for b in range(2):
            delta_hand(b, s, True).wait_recv()
    in_order(r.g_all, r.g_seq, 1)

    def order_delta(i):
        for b in range(2):
            r.delta_row[i, :, b * half : (b + 1) * half] = r.delta_all[r.table[1, 2 * i + b]]

    loop(0, count, order_delta)

    def keep(kind, n, target, value):
        mine = p.own(n, turn)
        target[2 * mine] = value[:half]
        target[2 * mine + 1] = value[half:]
        for s in range(1, share):
            kv_copy(kind, n, s, target, False).start()

    def value_pass(n):
        mine = p.own(n, turn)
        first = p.offset(n, turn) - mine

        def some(i, width, acc):
            probs = jnp.concatenate([r.cache[first + i + u] for u in range(width)], axis=1)
            return acc + dot_nn(probs, r.g_seq[pl.ds(pl.multiple_of(i * tok, tok), width * tok), :])

        acc = spans(mine, count, some, jnp.zeros((tok, HD), F32))
        keep(0, n, r.dv_seq, acc.astype(BF16))

    def kv_copy(kind, n, s, target, arriving):
        source = (turn - s + share) % share if arriving else turn
        rows = pair_at(p.own(n, source))
        return remote(
            target.at[rows],
            target.at[rows],
            r.sem_kv_s.at[kind, n, s],
            r.sem_kv_r.at[kind, n, s],
            head * share + (turn + s) % share,
        )

    def kv_arrive(kind, target):
        def one(n):
            for s in range(1, share):
                kv_copy(kind, n, s, target, True).wait_recv()

        loop(0, heads, one)

    outs = (r.out_q, r.out_k, r.out_v)

    def res_copy(kind, d):
        to = (head + d) % heads
        return remote(
            r.send.at[kind, d],
            outs[kind].at[:, :, cols(head)],
            r.sem_res_s.at[kind, d],
            r.sem_res_r.at[kind, d],
            to * share + turn,
        )

    def res_local(kind):
        return local(r.send.at[kind, 0], outs[kind].at[:, :, cols(head)], r.sem_out.at[kind])

    def hand_back(kind, value_of):
        def one(d):
            flat = (turn * heads + (head + d) % heads) * 2
            for b in range(2):
                place = place_of(flat + b)
                value = value_of(place, (head + d) % heads, b)
                r.send[kind, d, b] = value

        def both(d):
            one(d)
            res_copy(kind, d).start()

        loop(1, heads, both)
        one(0)
        res_local(kind).start()

    loop(0, heads, value_pass)
    kv_arrive(0, r.dv_seq)
    hand_back(2, lambda place, h, b: r.dv_seq[place])

    def score_pass(n):
        mine = p.own(n, turn)
        first = p.offset(n, turn) - mine
        keys = rows_at(mine, tok)

        def some(i, width, acc):
            scores = []
            for u in range(width):
                grad_prob = dot_nt(r.v_seq[keys, :], r.g_seq[rows_at(i + u, tok), :])
                change = grad_prob - r.delta_row[i + u, 0:1, :]
                score = (r.cache[first + i + u].astype(F32) * change).astype(BF16)
                r.dq_turn[i + u] += dot_nn(r.k_turn[n], score)
                scores.append(score)
            queries = r.q_seq[pl.ds(pl.multiple_of(i * tok, tok), width * tok), :]
            return acc + dot_nn(jnp.concatenate(scores, axis=1), queries)

        acc = spans(mine, count, some, jnp.zeros((tok, HD), F32))
        keep(1, n, r.dk_seq, (acc * SCALE).astype(BF16))

    loop(0, heads, score_pass)

    def turn_queries(i):
        value = r.dq_turn[i].T * SCALE
        r.dq_seq[2 * i] = value[:half]
        r.dq_seq[2 * i + 1] = value[half:]

    loop(0, count, turn_queries)

    def q_copy(s):
        return remote(
            r.dq_out.at[s - 1],
            r.dq_got.at[s - 1],
            r.sem_q_s.at[s],
            r.sem_q_r.at[s],
            head * share + (turn + s) % share,
        )

    for s in range(1, share):

        def pick(f, s=s):
            place = place_of((turn + s) % share * heads * 2 + f)
            r.dq_out[s - 1, f] = r.dq_seq[place]

        loop(0, 2 * heads, pick)
        q_copy(s).start()

    kv_arrive(1, r.dk_seq)
    hand_back(1, lambda place, h, b: r.dk_seq[place])
    for s in range(1, share):
        q_copy(s).wait_recv()

    def dq_value(place, h, b):
        value = r.dq_seq[place]
        for s in range(1, share):
            value = value + r.dq_got[s - 1, 2 * h + b]
        return value.astype(BF16)

    hand_back(0, dq_value)

    for n in range(p.chunks):
        for d in range(1, p.parts):
            dy_copy(d, n).wait_send()
    loop(1, near, lambda d: near_copy(d, False).wait_send())
    loop(1, far, lambda d: far_copy(d).wait_send())
    for i in range(3):
        loop(1, heads, lambda d, i=i: in_copy(i, d, False).wait_send())
        for s in range(1, share):
            hand_on(alls[i], i, s, False, fw).wait_send()
    for n in range(p.chunks):
        loop(1, heads, lambda d, n=n: g_copy(n, d, False).wait_send())
    for b in range(2):
        loop(1, heads, lambda d, b=b: delta_copy(b, d, False).wait_send())
    for s in range(1, share):
        for n in range(p.chunks):
            g_hand(n, s, False).wait_send()
        for b in range(2):
            delta_hand(b, s, False).wait_send()
        q_copy(s).wait_send()

        def kv_sent(n, s=s):
            kv_copy(0, n, s, r.dv_seq, False).wait_send()
            kv_copy(1, n, s, r.dk_seq, False).wait_send()

        loop(0, heads, kv_sent)
    for kind in range(3):
        loop(1, heads, lambda d, kind=kind: res_copy(kind, d).wait_send())
        loop(1, heads, lambda d, kind=kind: res_copy(kind, d).wait_recv())
        res_local(kind).wait()
    for c in give:
        c.wait()


def copy_kernel(*refs):
    sources, targets, held, (sem_in, sem_out) = refs[:6], refs[6:12], refs[12:18], refs[18:]
    into, out = [], []
    for i in range(6):
        size = held[i].shape[0] // 2
        for j in range(2):
            part = pl.ds(j * size, size)
            into.append(
                pltpu.make_async_copy(sources[i].at[part], held[i].at[part], sem_in.at[i, j])
            )
            out.append(
                pltpu.make_async_copy(held[i].at[part], targets[i].at[part], sem_out.at[i, j])
            )
    for c in into:
        c.start()
    for c, d in zip(into, out, strict=True):
        c.wait()
        d.start()
    for d in out:
        d.wait()


def body(
    attn_q,
    attn_k,
    attn_v,
    attn_o,
    attn_dy,
    out_weight,
    block_place,
    hyena_q,
    hyena_k,
    hyena_v,
    hyena_dy,
    filter_residue,
    filter_rate,
):
    tok, feat = attn_q.shape
    chan = hyena_q.shape[1]
    modes, groups = filter_rate.shape
    count, parts = lax.axis_size("ctx"), lax.axis_size("tp")
    p = Plan(count, parts, tok, feat, attn_dy.shape[1], chan, modes, groups)
    items = scratch(p)
    names = INPUTS + OUTPUTS + tuple(items)
    hbm = pl.BlockSpec(memory_space=pl.ANY)
    vmem = pl.BlockSpec(memory_space=pltpu.VMEM)
    attn_out = jax.ShapeDtypeStruct((2, p.half, feat), BF16)
    hy_out = jax.ShapeDtypeStruct((tok, chan), BF16)
    outs = pl.pallas_call(
        functools.partial(kernel, p, names),
        in_specs=[pl.BlockSpec(memory_space=pltpu.SMEM), vmem, vmem] + [hbm] * 10,
        out_specs=[hbm] * 6,
        out_shape=[attn_out] * 3 + [hy_out] * 3,
        scratch_shapes=list(items.values()),
        compiler_params=pltpu.CompilerParams(
            collective_id=0, has_side_effects=True, vmem_limit_bytes=63 * 1024 * 1024
        ),
        name="grads",
    )(
        block_place,
        filter_rate,
        filter_residue,
        attn_q.reshape(2, p.half, feat),
        attn_k.reshape(2, p.half, feat),
        attn_v.reshape(2, p.half, feat),
        attn_o,
        attn_dy,
        out_weight,
        hyena_q,
        hyena_k,
        hyena_v,
        hyena_dy,
    )
    outs = pl.pallas_call(
        copy_kernel,
        in_specs=[hbm] * 6,
        out_specs=[hbm] * 6,
        out_shape=[attn_out] * 3 + [hy_out] * 3,
        scratch_shapes=[pltpu.VMEM(attn_out.shape, BF16)] * 3
        + [pltpu.VMEM(hy_out.shape, BF16)] * 3
        + [pltpu.SemaphoreType.DMA((6, 2))] * 2,
        name="results",
    )(*outs)
    return tuple(x.reshape(tok, feat) for x in outs[:3]) + tuple(outs[3:])


def solution(mesh):
    both = P("ctx", "tp")
    in_specs = (both,) * 5 + (P("tp", None), P()) + (both,) * 4 + (P(None, "tp"),) * 2
    return jax.shard_map(body, mesh=mesh, in_specs=in_specs, out_specs=(both,) * 6, check_vma=False)
```

```python
import functools
import math

import jax
import jax.numpy as jnp
from jax import lax
from jax.experimental import pallas as pl
from jax.experimental.pallas import tpu as pltpu
from jax.sharding import PartitionSpec as P

HD = 128
NEG_LARGE = -1e30
F32 = jnp.float32
BF16 = jnp.bfloat16
MESH = pl.DeviceIdType.MESH
LN2_SCALE = HD ** (-0.5) * math.log2(math.e)
SCALE = HD ** (-0.5)


def dot_nn(a, b):
    return lax.dot_general(a, b, (((1,), (0,)), ((), ())), preferred_element_type=F32)


def dot_nt(a, b):
    return lax.dot_general(a, b, (((1,), (1,)), ((), ())), preferred_element_type=F32)


def split(x):
    high = x.astype(BF16)
    return high, (x - high.astype(F32)).astype(BF16)


def rows_at(block, size):
    return pl.ds(pl.multiple_of(block * size, size), size)


def loop(start, stop, fn):
    def step(i, carry):
        fn(i)
        return carry

    lax.fori_loop(start, stop, step, 0)


def spans(start, stop, fn, carry=0):
    for width in (4, 2, 1):
        turns = (stop - start) // width
        carry = lax.fori_loop(
            0, turns, lambda t, c, s=start, w=width: fn(s + w * t, w, c), carry
        )
        start = start + width * turns
    return carry


class Plan:
    def __init__(self, count, parts, tok, feat, width, chan, modes, groups):
        self.count, self.parts = count, parts
        self.tok, self.feat, self.width = tok, feat, width
        self.chan, self.modes, self.groups = chan, modes, groups
        self.heads = feat // HD
        self.share = count // self.heads
        self.half = tok // 2
        self.near = 4 if count % 4 == 0 else count
        self.far = count // self.near
        self.chunks = 4
        self.piece = tok // self.chunks
        self.tile = min(256, feat)
        self.size = chan // groups
        self.blocks = max(
            sum(count - self.own(n, turn) for n in range(self.heads)) for turn in range(self.share)
        )

    def own(self, n, turn):
        return n * self.share + turn + (n % 2) * (self.share - 1 - 2 * turn)

    def offset(self, n, turn):
        share = self.share
        before = (
            share * (n * (n - 1) // 2) + ((n + 1) // 2) * turn + (n // 2) * (share - 1 - turn)
        )
        return n * self.count - before

    def held(self, i, turn):
        at = i // self.share
        mine = self.own(at, turn) - at * self.share
        return at + (i % self.share - mine + self.share) // self.share


def scratch(p):
    vm = pltpu.VMEM
    total = p.count * p.tok
    low = vm((total, HD), BF16)
    blocked = vm((2 * p.count, p.half, HD), BF16)
    other = max(p.share - 1, 1)
    rest = max(p.parts - 1, 1)
    lines = p.groups * p.modes
    dma = pltpu.SemaphoreType.DMA

    def pair(*shape):
        return [dma(shape), dma(shape)]

    items = dict(
        dy_own=vm((p.tok, p.width), BF16),
        dy_got=vm((rest, p.tok, p.width), BF16),
        w_own=vm((p.feat, p.width), BF16),
        w_rest=vm((rest, p.feat, p.width), BF16),
        g_part=vm((p.tok, p.feat), F32),
        o_buf=vm((p.tok, p.feat), BF16),
        g_low=vm((p.tok, p.feat), BF16),
        table=pltpu.SMEM((2, 2 * p.count), jnp.int32),
        delta_out=vm((2, p.heads, 8, HD), F32),
        delta_all=vm((2 * p.count, 8, HD), F32),
        delta_row=vm((p.count, 8, p.tok), F32),
        q_all=blocked,
        k_all=blocked,
        v_all=blocked,
        g_all=blocked,
        q_seq=low,
        k_seq=low,
        v_seq=low,
        g_seq=low,
        k_turn=vm((p.heads, HD, p.tok), BF16),
        cache=vm((p.blocks, p.tok, p.tok), BF16),
        ml=vm((p.heads * p.count, 8, p.tok), F32),
        ml_own=vm((p.count, 8, p.tok), F32),
        ml_got=vm((other, p.count, 8, p.tok), F32),
        dq_seq=vm((2 * p.count, p.half, HD), F32),
        dq_out=vm((other, 2 * p.heads, p.half, HD), BF16),
        dq_got=vm((other, 2 * p.heads, p.half, HD), BF16),
        dk_seq=blocked,
        dv_seq=blocked,
        send=vm((3, p.heads, 2, p.half, HD), BF16),
        hy_in=vm((4, p.tok, p.chan), BF16),
        hy_out=vm((3, p.tok, p.chan), BF16),
        st_own=vm((2, lines, HD), BF16),
        st_got=vm((p.near, 2, lines, HD), BF16),
        st_far=vm((2, lines, HD), BF16),
        far_got=vm((max(p.far - 1, 1), lines, HD), BF16),
        st_fin=vm((2, lines, HD), F32),
        sem_local=dma((16,)),
        sem_rest=dma((rest,)),
        sem_out=dma((6,)),
        sem_dy_s=dma((rest, p.chunks)),
        sem_dy_r=dma((rest, p.chunks)),
        sem_in_s=dma((3, p.heads)),
        sem_in_r=dma((3, p.heads)),
        sem_fw_s=dma((3, p.heads, p.share)),
        sem_fw_r=dma((3, p.heads, p.share)),
        sem_g_s=dma((p.chunks, p.heads)),
        sem_g_r=dma((p.chunks, p.heads)),
        sem_gf_s=dma((p.chunks, p.share)),
        sem_gf_r=dma((p.chunks, p.share)),
        sem_d_s=dma((2, p.heads)),
        sem_d_r=dma((2, p.heads)),
        sem_df_s=dma((2, p.share)),
        sem_df_r=dma((2, p.share)),
        sem_st_s=dma((p.near,)),
        sem_st_r=dma((p.near,)),
        sem_far_s=dma((p.far,)),
        sem_far_r=dma((p.far,)),
        sem_ml_s=dma((p.share,)),
        sem_ml_r=dma((p.share,)),
        sem_kv_s=dma((2, p.heads, p.share)),
        sem_kv_r=dma((2, p.heads, p.share)),
        sem_q_s=dma((p.share,)),
        sem_q_r=dma((p.share,)),
        sem_res_s=dma((3, p.heads)),
        sem_res_r=dma((3, p.heads)),
    )
    return items


class Refs:
    pass


INPUTS = (
    "places",
    "rate",
    "res",
    "attn_q",
    "attn_k",
    "attn_v",
    "attn_o",
    "attn_dy",
    "weight",
    "hy_q",
    "hy_k",
    "hy_v",
    "hy_dy",
)
OUTPUTS = ("out_q", "out_k", "out_v", "out_hq", "out_hk", "out_hv")


def column(ref, g):
    x = ref[...]
    lane = lax.broadcasted_iota(jnp.int32, x.shape, 1)
    return jnp.sum(jnp.where(lane == g, x, 0.0), axis=1, keepdims=True)


def kernel(p, names, *refs):
    r = Refs()
    for name, ref in zip(names, refs, strict=True):
        setattr(r, name, ref)
    me = lax.axis_index("ctx").astype(jnp.int32)
    at = lax.axis_index("tp").astype(jnp.int32)
    count, heads, share, tok, half = p.count, p.heads, p.share, p.tok, p.half
    head, turn = me // share, me % share

    def remote(src, dst, send, recv, ctx):
        return pltpu.make_async_remote_copy(
            src_ref=src,
            dst_ref=dst,
            send_sem=send,
            recv_sem=recv,
            device_id={"ctx": ctx},
            device_id_type=MESH,
        )

    def local(src, dst, sem):
        return pltpu.make_async_copy(src, dst, sem)

    def cols(h):
        return rows_at(h, HD)

    def pair_at(i):
        return pl.ds(2 * i, 2)

    barrier = pltpu.get_barrier_semaphore()
    for d in range(1, count):
        pl.semaphore_signal(
            barrier, inc=1, device_id={"ctx": (me + d) % count}, device_id_type=MESH
        )
    for d in range(1, p.parts):
        pl.semaphore_signal(
            barrier, inc=1, device_id={"tp": (at + d) % p.parts}, device_id_type=MESH
        )
    pl.semaphore_wait(barrier, count + p.parts - 2)

    def dy_copy(d, n):
        rows = pl.ds(n * p.piece, p.piece)
        return pltpu.make_async_remote_copy(
            src_ref=r.attn_dy.at[rows, :],
            dst_ref=r.dy_got.at[d - 1, rows, :],
            send_sem=r.sem_dy_s.at[d - 1, n],
            recv_sem=r.sem_dy_r.at[d - 1, n],
            device_id={"tp": (at + d) % p.parts},
            device_id_type=MESH,
        )

    for n in range(p.chunks):
        for d in range(1, p.parts):
            dy_copy(d, n).start()

    def part_cols(d):
        return rows_at((at - d + p.parts) % p.parts, p.width)

    hy_src = (r.hy_q, r.hy_k, r.hy_v, r.hy_dy)
    fetch_hy = [local(hy_src[i], r.hy_in.at[i], r.sem_local.at[i]) for i in range(4)]
    fetch_dy = local(r.attn_dy, r.dy_own, r.sem_local.at[4])
    fetch_w = local(r.weight.at[:, part_cols(0)], r.w_own, r.sem_local.at[5])
    fetch_o = local(r.attn_o, r.o_buf, r.sem_local.at[6])
    sources = (r.attn_k, r.attn_q, r.attn_v)
    alls = (r.k_all, r.q_all, r.v_all)
    seqs = (r.k_seq, r.q_seq, r.v_seq)
    own_slot = pair_at(turn * heads + head)
    fetch_own = [
        local(sources[i].at[:, :, cols(head)], alls[i].at[own_slot], r.sem_local.at[7 + i])
        for i in range(3)
    ]
    for c in fetch_hy:
        c.start()
    fetch_dy.start()
    fetch_w.start()

    def in_copy(i, d, arriving):
        to = (head + d) % heads
        source = (head - d + heads) % heads if arriving else head
        slot = pair_at(turn * heads + source)
        return remote(
            sources[i].at[:, :, cols(to)],
            alls[i].at[slot],
            r.sem_in_s.at[i, d],
            r.sem_in_r.at[i, d],
            to * share + turn,
        )

    for i in range(2):
        loop(1, heads, lambda d, i=i: in_copy(i, d, False).start())
    for c in fetch_own:
        c.start()
    fetch_o.start()
    fetch_rest = []
    for d in range(1, p.parts):
        c = local(r.weight.at[:, part_cols(d)], r.w_rest.at[d - 1], r.sem_rest.at[d - 1])
        fetch_rest.append(c)

    for c in fetch_hy:
        c.wait()
    lane_shape = (p.modes, tok)
    lag = lax.broadcasted_iota(jnp.int32, lane_shape, 1).astype(F32)

    def hy_block(i, g):
        return r.hy_in[i, :, rows_at(g, p.size)].astype(F32)

    def twice(x):
        return jnp.concatenate(split(x), axis=1)

    def state_of(decay, prod):
        both = dot_nn(jnp.concatenate(split(decay), axis=0), twice(prod))
        both = both[: p.modes] + both[p.modes :]
        return both[:, : p.size] + both[:, p.size :]

    def one_state(g):
        rate = column(r.rate, g)
        tail = jnp.exp(-rate * (tok - 1 - lag))
        first = jnp.exp(-rate * lag)
        lines = rows_at(g, p.modes)
        r.st_own[0, lines, :] = state_of(tail, hy_block(1, g) * hy_block(2, g)).astype(BF16)
        r.st_own[1, lines, :] = state_of(first, hy_block(0, g) * hy_block(3, g)).astype(BF16)

    loop(0, p.groups, one_state)

    near, far = p.near, p.far
    my_near, my_far = me % near, me // near

    def near_copy(d, arriving):
        source = (my_near - d + near) % near if arriving else my_near
        return remote(
            r.st_own,
            r.st_got.at[source],
            r.sem_st_s.at[d],
            r.sem_st_r.at[d],
            my_far * near + (my_near + d) % near,
        )

    loop(1, near, lambda d: near_copy(d, False).start())

    fetch_dy.wait()
    fetch_w.wait()
    for c in fetch_rest:
        c.start()

    def own_product(n):
        at_cols = rows_at(n, p.tile)
        r.g_part[:, at_cols] = dot_nt(r.dy_own[...], r.w_own[at_cols, :])

    loop(0, p.feat // p.tile, own_product)

    def place_of(flat):
        source, h = flat // (2 * heads), flat // 2 % heads
        return r.places[(h * share + source) * 2 + flat % 2]

    def find(place):
        slot = jnp.int32(0)
        for stored in range(2 * count):
            c, b = divmod(stored, 2)
            flat = c % share * heads + c // share
            slot = jnp.where(r.places[stored] == place, 2 * flat + b, slot)
        r.table[0, place] = slot
        r.table[1, place] = slot % 2 * count + slot // 2

    loop(0, 2 * count, find)

    row_id = lax.broadcasted_iota(jnp.int32, (8, tok), 0)
    empty = jnp.where(row_id == 0, NEG_LARGE, 0.0)

    def clear(n):
        r.ml[n] = empty

    loop(0, heads * count, clear)

    def hand_on(i, d, s, arriving):
        source = (turn - s + share) % share if arriving else turn
        slot = pair_at(source * heads + (head - d + heads) % heads)
        return remote(
            alls[i].at[slot],
            alls[i].at[slot],
            r.sem_fw_s.at[i, d, s],
            r.sem_fw_r.at[i, d, s],
            head * share + (turn + s) % share,
        )

    def arrive(*kinds):
        for i in kinds:
            fetch_own[i].wait()
            for s in range(1, share):
                hand_on(i, 0, s, False).start()

        def one(d):
            for i in kinds:
                in_copy(i, d, True).wait_recv()
                for s in range(1, share):
                    hand_on(i, d, s, False).start()

        loop(1, heads, one)

    def in_order(source, target, row):
        def one(place):
            target[rows_at(place, half), :] = source[r.table[row, place]]

        loop(0, 2 * count, one)

    def settle(i):
        for s in range(1, share):
            loop(0, heads, lambda d, s=s: hand_on(i, d, s, True).wait_recv())
        in_order(alls[i], seqs[i], 0)

    def g_place(n, source):
        slot, start = divmod(n * p.piece, half)
        return slot * count + turn * heads + source, pl.ds(start, p.piece)

    def g_copy(n, d, arriving):
        to = (head + d) % heads
        source = (head - d + heads) % heads if arriving else head
        rows = pl.ds(n * p.piece, p.piece)
        slot, inner = g_place(n, source)
        return remote(
            r.g_low.at[rows, cols(to)],
            r.g_all.at[slot, inner, :],
            r.sem_g_s.at[n, d],
            r.sem_g_r.at[n, d],
            to * share + turn,
        )

    def g_chunks(start, stop):
        for n in range(start, stop):
            for d in range(1, p.parts):
                dy_copy(d, n).wait_recv()
        rows = pl.ds(start * p.piece, (stop - start) * p.piece)

        def tile(c):
            at_cols = rows_at(c, p.tile)
            total = r.g_part[rows, at_cols]
            for d in range(1, p.parts):
                total = total + dot_nt(r.dy_got[d - 1, rows, :], r.w_rest[d - 1, at_cols, :])
            r.g_low[rows, at_cols] = total.astype(BF16)

        loop(0, p.feat // p.tile, tile)
        for n in range(start, stop):
            loop(1, heads, lambda d, n=n: g_copy(n, d, False).start())
        for n in range(start, stop):
            slot, inner = g_place(n, head)
            r.g_all[slot, inner, :] = r.g_low[pl.ds(n * p.piece, p.piece), cols(head)]

    def g_hand(n, s, arriving):
        source = (turn - s + share) % share if arriving else turn
        slot, start = divmod(n * p.piece, half)
        part = r.g_all.at[
            pl.ds(slot * count + source * heads, heads), pl.ds(start, p.piece), :
        ]
        return remote(
            part,
            part,
            r.sem_gf_s.at[n, s],
            r.sem_gf_r.at[n, s],
            head * share + (turn + s) % share,
        )

    def g_arrive(n):
        loop(1, heads, lambda d: g_copy(n, d, True).wait_recv())
        for s in range(1, share):
            g_hand(n, s, False).start()

    ones = jnp.ones((8, HD), BF16)

    def delta_copy(b, d, arriving):
        to = (head + d) % heads
        source = (head - d + heads) % heads if arriving else head
        return remote(
            r.delta_out.at[b, to],
            r.delta_all.at[b * count + turn * heads + source],
            r.sem_d_s.at[b, d],
            r.sem_d_r.at[b, d],
            to * share + turn,
        )

    def delta_half(b):
        rows = pl.ds(b * half, half)

        def one(h):
            prod = r.g_low[rows, cols(h)].astype(F32) * r.o_buf[rows, cols(h)].astype(F32)
            high, low = split(prod)
            r.delta_out[b, h] = dot_nt(ones, high) + dot_nt(ones, low)

        loop(0, heads, one)
        loop(1, heads, lambda d: delta_copy(b, d, False).start())
        r.delta_all[b * count + turn * heads + head] = r.delta_out[b, head]

    def delta_hand(b, s, arriving):
        source = (turn - s + share) % share if arriving else turn
        part = r.delta_all.at[pl.ds(b * count + source * heads, heads)]
        return remote(
            part,
            part,
            r.sem_df_s.at[b, s],
            r.sem_df_r.at[b, s],
            head * share + (turn + s) % share,
        )

    def delta_arrive(b):
        loop(1, heads, lambda d: delta_copy(b, d, True).wait_recv())
        for s in range(1, share):
            delta_hand(b, s, False).start()

    square = (tok, tok)

    def turn_keys(n):
        mine = p.own(n, turn)
        r.k_turn[n] = r.k_seq[rows_at(mine, tok), :].astype(F32).T.astype(BF16)

    def spread(n):
        mine = p.own(n, turn)
        first = p.offset(n, turn)
        keys = rows_at(mine, tok)

        def one(i, masked=False):
            s = dot_nt(r.k_seq[keys, :], r.q_seq[rows_at(i, tok), :])
            if masked:
                key_id = lax.broadcasted_iota(jnp.int32, square, 0)
                query_id = lax.broadcasted_iota(jnp.int32, square, 1)
                s = jnp.where(key_id <= query_id, s, NEG_LARGE)
            peak = jnp.max(s, axis=0, keepdims=True)
            e = jnp.exp2((s - peak) * LN2_SCALE)
            r.cache[first + i - mine] = e.astype(BF16)
            r.ml[n * count + i, 0:1, :] = peak
            r.ml[n * count + i, 1:2, :] = jnp.sum(e, axis=0, keepdims=True)

        def some(i, width, carry):
            for u in range(width):
                one(i + u)
            return carry

        one(mine, True)
        spans(mine + 1, count, some)

    def combine(i):
        peaks = [r.ml[n * count + i, 0:1, :] for n in range(heads)]
        peak = functools.reduce(jnp.maximum, peaks)
        total = 0.0
        for n in range(heads):
            weight = jnp.exp2((peaks[n] - peak) * LN2_SCALE)
            total = total + weight * r.ml[n * count + i, 1:2, :]
        r.ml_own[i] = empty
        r.ml_own[i, 0:1, :] = peak
        r.ml_own[i, 1:2, :] = total

    def ml_copy(s):
        return remote(
            r.ml_own,
            r.ml_got.at[s - 1],
            r.sem_ml_s.at[s],
            r.sem_ml_r.at[s],
            head * share + (turn + s) % share,
        )

    def join(i):
        peaks = [r.ml_own[i, 0:1, :]] + [r.ml_got[s, i, 0:1, :] for s in range(share - 1)]
        peak = functools.reduce(jnp.maximum, peaks)
        total = jnp.exp2((peaks[0] - peak) * LN2_SCALE) * r.ml_own[i, 1:2, :]
        for s in range(share - 1):
            weight = jnp.exp2((peaks[s + 1] - peak) * LN2_SCALE)
            total = total + weight * r.ml_got[s, i, 1:2, :]
        r.ml_own[i, 0:1, :] = peak
        r.ml_own[i, 1:2, :] = 1.0 / total

    def normal(n):
        mine = p.own(n, turn)
        first = p.offset(n, turn)

        def one(i):
            weight = jnp.exp2((r.ml[n * count + i, 0:1, :] - r.ml_own[i, 0:1, :]) * LN2_SCALE)
            weight = weight * r.ml_own[i, 1:2, :]
            e = r.cache[first + i - mine].astype(F32)
            r.cache[first + i - mine] = (e * weight).astype(BF16)

        loop(mine, count, one)

    def decay(rate, steps, good):
        power = jnp.exp(-rate * (tok * jnp.maximum(steps, 0)).astype(F32))
        return jnp.where(good, power, 0.0)

    def near_sum(g):
        rate = column(r.rate, g)
        lines = rows_at(g, p.modes)
        zero = jnp.zeros((p.modes, p.size), F32)
        total, back, fin, fin_back = zero, zero, zero, zero
        for other in range(near):
            ahead = r.st_got[other, 0, lines, :].astype(F32)
            behind = r.st_got[other, 1, lines, :].astype(F32)
            total = total + decay(rate, jnp.int32(near - 1 - other), True) * ahead
            back = back + decay(rate, jnp.int32(other), True) * behind
            gap = my_near - 1 - other
            fin = fin + decay(rate, gap, gap >= 0) * ahead
            gap = other - 1 - my_near
            fin_back = fin_back + decay(rate, gap, gap >= 0) * behind
        r.st_far[0, lines, :] = total.astype(BF16)
        r.st_far[1, lines, :] = back.astype(BF16)
        r.st_fin[0, lines, :] = fin
        r.st_fin[1, lines, :] = fin_back

    def far_copy(d):
        to = (my_far + d) % far
        return remote(
            r.st_far.at[(my_far + d) // far],
            r.far_got.at[d - 1],
            r.sem_far_s.at[d],
            r.sem_far_r.at[d],
            to * near + my_near,
        )

    def far_sum(g):
        rate = column(r.rate, g)
        lines = rows_at(g, p.modes)
        ahead = jnp.zeros((p.modes, p.size), F32)
        behind = ahead
        for d in range(1, far):
            got = r.far_got[d - 1, lines, :].astype(F32)
            source = (my_far - d + far) % far
            gap = (my_far - 1 - source) * near + my_near
            ahead = ahead + decay(rate, gap, source < my_far) * got
            gap = (source - 1 - my_far) * near + near - 1 - my_near
            behind = behind + decay(rate, gap, source > my_far) * got
        r.st_fin[0, lines, :] += ahead
        r.st_fin[1, lines, :] += behind

    lag_id = lax.broadcasted_iota(jnp.int32, lane_shape, 1)
    turned = jnp.where(lag_id == 0, 0, tok - lag_id).astype(F32)
    tall = (half, tok)
    row = lax.broadcasted_iota(jnp.int32, (half, half), 0)
    col = lax.broadcasted_iota(jnp.int32, (half, half), 1)
    blank = jnp.zeros((half, half), F32)

    def mixed(bands, prod, edge, state):
        high, low = split(bands)
        pair = twice(prod)
        out = dot_nn(high, pair) + dot_nn(low, pair)
        e_high = edge.astype(BF16).astype(F32)
        s_high, s_low = split(state)
        left = jnp.concatenate([e_high, edge - e_high, e_high], axis=0).T.astype(BF16)
        right = jnp.concatenate([s_high, s_high, s_low], axis=0)
        return out[:, : p.size] + out[:, p.size :] + dot_nn(left, right)

    def mix(g):
        rate = jnp.broadcast_to(column(r.rate, g), lane_shape)
        res = jnp.broadcast_to(column(r.res, g), lane_shape)
        taps = jnp.sum(res * jnp.exp(-rate * lag), axis=0, keepdims=True)
        back_taps = jnp.sum(res * jnp.exp(-rate * turned), axis=0, keepdims=True)
        lower = pltpu.roll(jnp.broadcast_to(back_taps, tall), 0, 1, stride=1, stride_axis=0)
        upper = pltpu.roll(jnp.broadcast_to(taps, tall), 0, 1, stride=1, stride_axis=0)
        near_low = jnp.where(col <= row, lower[:, :half], 0.0)
        near_up = jnp.where(col >= row, upper[:, :half], 0.0)
        lower = jnp.concatenate(
            [
                jnp.concatenate([near_low, blank], axis=1),
                jnp.concatenate([lower[:, half:], near_low], axis=1),
            ],
            axis=0,
        )
        upper = jnp.concatenate(
            [
                jnp.concatenate([near_up, upper[:, half:]], axis=1),
                jnp.concatenate([blank, near_up], axis=1),
            ],
            axis=0,
        )
        lines = rows_at(g, p.modes)
        into = res * jnp.exp(-rate * (lag + 1.0))
        back = res * jnp.exp(-rate * (tok - lag))
        k, v, dy = hy_block(1, g), hy_block(2, g), hy_block(3, g)
        conv = mixed(lower, k * v, into, r.st_fin[0, lines, :])
        mid = mixed(upper, hy_block(0, g) * dy, back, r.st_fin[1, lines, :])
        here = rows_at(g, p.size)
        r.hy_out[0, :, here] = (dy * conv).astype(BF16)
        r.hy_out[1, :, here] = (mid * v).astype(BF16)
        r.hy_out[2, :, here] = (mid * k).astype(BF16)

    hy_outs = (r.out_hq, r.out_hk, r.out_hv)
    give = [local(r.hy_out.at[i], hy_outs[i], r.sem_out.at[3 + i]) for i in range(3)]

    arrive(0, 1)
    loop(1, heads, lambda d: in_copy(2, d, False).start())
    loop(1, near, lambda d: near_copy(d, True).wait_recv())
    r.st_got[my_near] = r.st_own[...]
    loop(0, p.groups, near_sum)
    loop(1, far, lambda d: far_copy(d).start())
    settle(0)
    settle(1)
    loop(0, heads, turn_keys)
    loop(0, heads, spread)
    loop(0, count, combine)
    for s in range(1, share):
        ml_copy(s).start()
    for c in fetch_rest:
        c.wait()
    last = p.chunks - 1
    g_chunks(0, last)
    fetch_o.wait()
    delta_half(0)
    arrive(2)
    for s in range(1, share):
        ml_copy(s).wait_recv()
        ml_copy(s).wait_send()
    loop(0, count, join)
    loop(0, heads, normal)
    g_chunks(last, p.chunks)
    delta_half(1)
    settle(2)
    for n in range(last):
        g_arrive(n)
    delta_arrive(0)
    g_arrive(last)
    delta_arrive(1)
    for s in range(1, share):
        for n in range(p.chunks):
            g_hand(n, s, True).wait_recv()
        for b in range(2):
            delta_hand(b, s, True).wait_recv()
    in_order(r.g_all, r.g_seq, 1)

    def order_delta(i):
        for b in range(2):
            r.delta_row[i, :, b * half : (b + 1) * half] = r.delta_all[r.table[1, 2 * i + b]]

    loop(0, count, order_delta)

    def keep(kind, n, target, value):
        mine = p.own(n, turn)
        target[2 * mine] = value[:half]
        target[2 * mine + 1] = value[half:]
        for s in range(1, share):
            kv_copy(kind, n, s, target, False).start()

    def value_pass(n):
        mine = p.own(n, turn)
        first = p.offset(n, turn) - mine

        def some(i, width, acc):
            probs = jnp.concatenate([r.cache[first + i + u] for u in range(width)], axis=1)
            return acc + dot_nn(probs, r.g_seq[pl.ds(pl.multiple_of(i * tok, tok), width * tok), :])

        acc = spans(mine, count, some, jnp.zeros((tok, HD), F32))
        keep(0, n, r.dv_seq, acc.astype(BF16))

    def kv_copy(kind, n, s, target, arriving):
        source = (turn - s + share) % share if arriving else turn
        rows = pair_at(p.own(n, source))
        return remote(
            target.at[rows],
            target.at[rows],
            r.sem_kv_s.at[kind, n, s],
            r.sem_kv_r.at[kind, n, s],
            head * share + (turn + s) % share,
        )

    def kv_arrive(kind, target):
        def one(n):
            for s in range(1, share):
                kv_copy(kind, n, s, target, True).wait_recv()

        loop(0, heads, one)

    outs = (r.out_q, r.out_k, r.out_v)

    def res_copy(kind, d):
        to = (head + d) % heads
        return remote(
            r.send.at[kind, d],
            outs[kind].at[:, :, cols(head)],
            r.sem_res_s.at[kind, d],
            r.sem_res_r.at[kind, d],
            to * share + turn,
        )

    def res_local(kind):
        return local(r.send.at[kind, 0], outs[kind].at[:, :, cols(head)], r.sem_out.at[kind])

    def hand_back(kind, value_of):
        def one(d):
            flat = (turn * heads + (head + d) % heads) * 2
            for b in range(2):
                place = place_of(flat + b)
                value = value_of(place, (head + d) % heads, b)
                r.send[kind, d, b] = value

        def both(d):
            one(d)
            res_copy(kind, d).start()

        loop(1, heads, both)
        one(0)
        res_local(kind).start()

    loop(0, heads, value_pass)
    kv_arrive(0, r.dv_seq)
    hand_back(2, lambda place, h, b: r.dv_seq[place])

    def score_pass(n):
        mine = p.own(n, turn)
        first = p.offset(n, turn) - mine
        keys = rows_at(mine, tok)

        def some(i, width, acc):
            scores = []
            for u in range(width):
                grad_prob = dot_nt(r.v_seq[keys, :], r.g_seq[rows_at(i + u, tok), :])
                change = grad_prob - r.delta_row[i + u, 0:1, :]
                score = (r.cache[first + i + u].astype(F32) * change).astype(BF16)
                r.cache[first + i + u] = score
                scores.append(score)
            queries = r.q_seq[pl.ds(pl.multiple_of(i * tok, tok), width * tok), :]
            return acc + dot_nn(jnp.concatenate(scores, axis=1), queries)

        acc = spans(mine, count, some, jnp.zeros((tok, HD), F32))
        keep(1, n, r.dk_seq, (acc * SCALE).astype(BF16))

    loop(0, heads, score_pass)
    kv_arrive(1, r.dk_seq)
    hand_back(1, lambda place, h, b: r.dk_seq[place])

    def query_pass(i):
        def some(n, width, acc):
            turned, scores = [], []
            for u in range(width):
                turned.append(r.k_turn[n + u])
                scores.append(r.cache[p.offset(n + u, turn) + i - p.own(n + u, turn)])
            left, right = jnp.concatenate(turned, axis=1), jnp.concatenate(scores, axis=0)
            return acc + dot_nn(left, right)

        acc = spans(0, p.held(i, turn), some, jnp.zeros((HD, tok), F32))
        value = acc.T * SCALE
        r.dq_seq[2 * i] = value[:half]
        r.dq_seq[2 * i + 1] = value[half:]

    loop(0, count, query_pass)

    def q_copy(s):
        return remote(
            r.dq_out.at[s - 1],
            r.dq_got.at[s - 1],
            r.sem_q_s.at[s],
            r.sem_q_r.at[s],
            head * share + (turn + s) % share,
        )

    for s in range(1, share):

        def pick(f, s=s):
            place = place_of((turn + s) % share * heads * 2 + f)
            r.dq_out[s - 1, f] = r.dq_seq[place].astype(BF16)

        loop(0, 2 * heads, pick)
        q_copy(s).start()

    loop(1, far, lambda d: far_copy(d).wait_recv())
    loop(0, p.groups, far_sum)
    loop(0, p.groups // 2, mix)
    for s in range(1, share):
        q_copy(s).wait_recv()

    def dq_value(place, h, b):
        value = r.dq_seq[place]
        for s in range(1, share):
            value = value + r.dq_got[s - 1, 2 * h + b].astype(F32)
        return value.astype(BF16)

    hand_back(0, dq_value)
    loop(p.groups // 2, p.groups, mix)
    for c in give:
        c.start()

    for n in range(p.chunks):
        for d in range(1, p.parts):
            dy_copy(d, n).wait_send()
    loop(1, near, lambda d: near_copy(d, False).wait_send())
    loop(1, far, lambda d: far_copy(d).wait_send())
    for i in range(3):
        loop(1, heads, lambda d, i=i: in_copy(i, d, False).wait_send())
        for s in range(1, share):
            loop(0, heads, lambda d, i=i, s=s: hand_on(i, d, s, False).wait_send())
    for n in range(p.chunks):
        loop(1, heads, lambda d, n=n: g_copy(n, d, False).wait_send())
    for b in range(2):
        loop(1, heads, lambda d, b=b: delta_copy(b, d, False).wait_send())
    for s in range(1, share):
        for n in range(p.chunks):
            g_hand(n, s, False).wait_send()
        for b in range(2):
            delta_hand(b, s, False).wait_send()
        q_copy(s).wait_send()

        def kv_sent(n, s=s):
            kv_copy(0, n, s, r.dv_seq, False).wait_send()
            kv_copy(1, n, s, r.dk_seq, False).wait_send()

        loop(0, heads, kv_sent)
    for kind in range(3):
        loop(1, heads, lambda d, kind=kind: res_copy(kind, d).wait_send())
        loop(1, heads, lambda d, kind=kind: res_copy(kind, d).wait_recv())
        res_local(kind).wait()
    for c in give:
        c.wait()


def copy_kernel(*refs):
    sources, targets, held, (sem_in, sem_out) = refs[:6], refs[6:12], refs[12:18], refs[18:]
    into, out = [], []
    for i in range(6):
        size = held[i].shape[0] // 2
        for j in range(2):
            part = pl.ds(j * size, size)
            into.append(
                pltpu.make_async_copy(sources[i].at[part], held[i].at[part], sem_in.at[i, j])
            )
            out.append(
                pltpu.make_async_copy(held[i].at[part], targets[i].at[part], sem_out.at[i, j])
            )
    for c in into:
        c.start()
    for c, d in zip(into, out, strict=True):
        c.wait()
        d.start()
    for d in out:
        d.wait()


def body(
    attn_q,
    attn_k,
    attn_v,
    attn_o,
    attn_dy,
    out_weight,
    block_place,
    hyena_q,
    hyena_k,
    hyena_v,
    hyena_dy,
    filter_residue,
    filter_rate,
):
    tok, feat = attn_q.shape
    chan = hyena_q.shape[1]
    modes, groups = filter_rate.shape
    count, parts = lax.axis_size("ctx"), lax.axis_size("tp")
    p = Plan(count, parts, tok, feat, attn_dy.shape[1], chan, modes, groups)
    items = scratch(p)
    names = INPUTS + OUTPUTS + tuple(items)
    hbm = pl.BlockSpec(memory_space=pl.ANY)
    vmem = pl.BlockSpec(memory_space=pltpu.VMEM)
    attn_out = jax.ShapeDtypeStruct((2, p.half, feat), BF16)
    hy_out = jax.ShapeDtypeStruct((tok, chan), BF16)
    outs = pl.pallas_call(
        functools.partial(kernel, p, names),
        in_specs=[pl.BlockSpec(memory_space=pltpu.SMEM), vmem, vmem] + [hbm] * 10,
        out_specs=[hbm] * 6,
        out_shape=[attn_out] * 3 + [hy_out] * 3,
        scratch_shapes=list(items.values()),
        compiler_params=pltpu.CompilerParams(
            collective_id=0, has_side_effects=True, vmem_limit_bytes=63 * 1024 * 1024
        ),
        name="grads",
    )(
        block_place,
        filter_rate,
        filter_residue,
        attn_q.reshape(2, p.half, feat),
        attn_k.reshape(2, p.half, feat),
        attn_v.reshape(2, p.half, feat),
        attn_o,
        attn_dy,
        out_weight,
        hyena_q,
        hyena_k,
        hyena_v,
        hyena_dy,
    )
    outs = pl.pallas_call(
        copy_kernel,
        in_specs=[hbm] * 6,
        out_specs=[hbm] * 6,
        out_shape=[attn_out] * 3 + [hy_out] * 3,
        scratch_shapes=[pltpu.VMEM(attn_out.shape, BF16)] * 3
        + [pltpu.VMEM(hy_out.shape, BF16)] * 3
        + [pltpu.SemaphoreType.DMA((6, 2))] * 2,
        name="results",
    )(*outs)
    return tuple(x.reshape(tok, feat) for x in outs[:3]) + tuple(outs[3:])


def solution(mesh):
    both = P("ctx", "tp")
    in_specs = (both,) * 5 + (P("tp", None), P()) + (both,) * 4 + (P(None, "tp"),) * 2
    return jax.shard_map(body, mesh=mesh, in_specs=in_specs, out_specs=(both,) * 6, check_vma=False)
```

```python
import functools
import math

import jax
import jax.numpy as jnp
from jax import lax
from jax.experimental import pallas as pl
from jax.experimental.pallas import tpu as pltpu
from jax.sharding import PartitionSpec as P

HD = 128
NEG_LARGE = -1e30
F32 = jnp.float32
BF16 = jnp.bfloat16
MESH = pl.DeviceIdType.MESH
LN2_SCALE = HD ** (-0.5) * math.log2(math.e)
SCALE = HD ** (-0.5)


def dot_nn(a, b):
    return lax.dot_general(a, b, (((1,), (0,)), ((), ())), preferred_element_type=F32)


def dot_nt(a, b):
    return lax.dot_general(a, b, (((1,), (1,)), ((), ())), preferred_element_type=F32)


def split(x):
    high = x.astype(BF16)
    return high, (x - high.astype(F32)).astype(BF16)


def rows_at(block, size):
    return pl.ds(pl.multiple_of(block * size, size), size)


def loop(start, stop, fn):
    def step(i, carry):
        fn(i)
        return carry

    lax.fori_loop(start, stop, step, 0)


def spans(start, stop, fn, carry=0):
    for width in (4, 2, 1):
        turns = (stop - start) // width
        carry = lax.fori_loop(
            0, turns, lambda t, c, s=start, w=width: fn(s + w * t, w, c), carry
        )
        start = start + width * turns
    return carry


class Plan:
    def __init__(self, count, parts, tok, feat, width, chan, modes, groups):
        self.count, self.parts = count, parts
        self.tok, self.feat, self.width = tok, feat, width
        self.chan, self.modes, self.groups = chan, modes, groups
        self.heads = feat // HD
        self.share = count // self.heads
        self.half = tok // 2
        self.near = 4 if count % 4 == 0 else count
        self.far = count // self.near
        self.chunks = 4
        self.piece = tok // self.chunks
        self.tile = min(256, feat)
        self.size = chan // groups
        self.blocks = max(
            sum(count - self.own(n, turn) for n in range(self.heads)) for turn in range(self.share)
        )

    def own(self, n, turn):
        return n * self.share + turn + (n % 2) * (self.share - 1 - 2 * turn)

    def offset(self, n, turn):
        share = self.share
        before = (
            share * (n * (n - 1) // 2) + ((n + 1) // 2) * turn + (n // 2) * (share - 1 - turn)
        )
        return n * self.count - before

    def held(self, i, turn):
        at = i // self.share
        mine = self.own(at, turn) - at * self.share
        return at + (i % self.share - mine + self.share) // self.share


def scratch(p):
    vm = pltpu.VMEM
    total = p.count * p.tok
    low = vm((total, HD), BF16)
    blocked = vm((2 * p.count, p.half, HD), BF16)
    other = max(p.share - 1, 1)
    rest = max(p.parts - 1, 1)
    lines = p.groups * p.modes
    dma = pltpu.SemaphoreType.DMA

    def pair(*shape):
        return [dma(shape), dma(shape)]

    items = dict(
        dy_own=vm((p.tok, p.width), BF16),
        dy_got=vm((rest, p.tok, p.width), BF16),
        w_own=vm((p.feat, p.width), BF16),
        w_rest=vm((rest, p.feat, p.width), BF16),
        g_part=vm((p.tok, p.feat), F32),
        o_buf=vm((p.tok, p.feat), BF16),
        g_low=vm((p.tok, p.feat), BF16),
        table=pltpu.SMEM((2, 2 * p.count), jnp.int32),
        delta_out=vm((2, p.heads, 8, HD), F32),
        delta_all=vm((2 * p.count, 8, HD), F32),
        delta_row=vm((p.count, 8, p.tok), F32),
        q_all=blocked,
        k_all=blocked,
        v_all=blocked,
        g_all=blocked,
        q_seq=low,
        k_seq=low,
        v_seq=low,
        g_seq=low,
        k_turn=vm((p.heads, HD, p.tok), BF16),
        cache=vm((p.blocks, p.tok, p.tok), BF16),
        ml=vm((p.heads * p.count, 8, p.tok), F32),
        ml_own=vm((p.count, 8, p.tok), F32),
        ml_got=vm((other, p.count, 8, p.tok), F32),
        dq_seq=vm((2 * p.count, p.half, HD), F32),
        dq_out=vm((other, 2 * p.heads, p.half, HD), BF16),
        dq_got=vm((other, 2 * p.heads, p.half, HD), BF16),
        dk_seq=blocked,
        dv_seq=blocked,
        send=vm((3, p.heads, 2, p.half, HD), BF16),
        hy_in=vm((4, p.tok, p.chan), BF16),
        hy_out=vm((3, p.tok, p.chan), BF16),
        st_own=vm((2, lines, HD), BF16),
        st_got=vm((p.near, 2, lines, HD), BF16),
        st_far=vm((2, lines, HD), BF16),
        far_got=vm((max(p.far - 1, 1), lines, HD), BF16),
        st_fin=vm((2, lines, HD), F32),
        sem_local=dma((16,)),
        sem_rest=dma((rest,)),
        sem_out=dma((6,)),
        sem_dy_s=dma((rest, p.chunks)),
        sem_dy_r=dma((rest, p.chunks)),
        sem_in_s=dma((3, p.heads)),
        sem_in_r=dma((3, p.heads)),
        sem_fw_s=dma((3, p.heads, p.share)),
        sem_fw_r=dma((3, p.heads, p.share)),
        sem_g_s=dma((p.chunks, p.heads)),
        sem_g_r=dma((p.chunks, p.heads)),
        sem_gf_s=dma((p.chunks, p.share)),
        sem_gf_r=dma((p.chunks, p.share)),
        sem_d_s=dma((2, p.heads)),
        sem_d_r=dma((2, p.heads)),
        sem_df_s=dma((2, p.share)),
        sem_df_r=dma((2, p.share)),
        sem_st_s=dma((p.near,)),
        sem_st_r=dma((p.near,)),
        sem_far_s=dma((p.far,)),
        sem_far_r=dma((p.far,)),
        sem_ml_s=dma((p.share,)),
        sem_ml_r=dma((p.share,)),
        sem_kv_s=dma((2, p.heads, p.share)),
        sem_kv_r=dma((2, p.heads, p.share)),
        sem_q_s=dma((p.share,)),
        sem_q_r=dma((p.share,)),
        sem_res_s=dma((3, p.heads)),
        sem_res_r=dma((3, p.heads)),
    )
    return items


class Refs:
    pass


INPUTS = (
    "places",
    "rate",
    "res",
    "attn_q",
    "attn_k",
    "attn_v",
    "attn_o",
    "attn_dy",
    "weight",
    "hy_q",
    "hy_k",
    "hy_v",
    "hy_dy",
)
OUTPUTS = ("out_q", "out_k", "out_v", "out_hq", "out_hk", "out_hv")


def column(ref, g):
    x = ref[...]
    lane = lax.broadcasted_iota(jnp.int32, x.shape, 1)
    return jnp.sum(jnp.where(lane == g, x, 0.0), axis=1, keepdims=True)


def kernel(p, names, *refs):
    r = Refs()
    for name, ref in zip(names, refs, strict=True):
        setattr(r, name, ref)
    me = lax.axis_index("ctx").astype(jnp.int32)
    at = lax.axis_index("tp").astype(jnp.int32)
    count, heads, share, tok, half = p.count, p.heads, p.share, p.tok, p.half
    head, turn = me // share, me % share

    def remote(src, dst, send, recv, ctx):
        return pltpu.make_async_remote_copy(
            src_ref=src,
            dst_ref=dst,
            send_sem=send,
            recv_sem=recv,
            device_id={"ctx": ctx},
            device_id_type=MESH,
        )

    def local(src, dst, sem):
        return pltpu.make_async_copy(src, dst, sem)

    def cols(h):
        return rows_at(h, HD)

    def pair_at(i):
        return pl.ds(2 * i, 2)

    barrier = pltpu.get_barrier_semaphore()
    for d in range(1, count):
        pl.semaphore_signal(
            barrier, inc=1, device_id={"ctx": (me + d) % count}, device_id_type=MESH
        )
    for d in range(1, p.parts):
        pl.semaphore_signal(
            barrier, inc=1, device_id={"tp": (at + d) % p.parts}, device_id_type=MESH
        )
    pl.semaphore_wait(barrier, count + p.parts - 2)

    def dy_copy(d, n):
        rows = pl.ds(n * p.piece, p.piece)
        return pltpu.make_async_remote_copy(
            src_ref=r.attn_dy.at[rows, :],
            dst_ref=r.dy_got.at[d - 1, rows, :],
            send_sem=r.sem_dy_s.at[d - 1, n],
            recv_sem=r.sem_dy_r.at[d - 1, n],
            device_id={"tp": (at + d) % p.parts},
            device_id_type=MESH,
        )

    for n in range(p.chunks):
        for d in range(1, p.parts):
            dy_copy(d, n).start()

    def part_cols(d):
        return rows_at((at - d + p.parts) % p.parts, p.width)

    hy_src = (r.hy_q, r.hy_k, r.hy_v, r.hy_dy)
    fetch_hy = [local(hy_src[i], r.hy_in.at[i], r.sem_local.at[i]) for i in range(4)]
    fetch_dy = local(r.attn_dy, r.dy_own, r.sem_local.at[4])
    fetch_w = local(r.weight.at[:, part_cols(0)], r.w_own, r.sem_local.at[5])
    fetch_o = local(r.attn_o, r.o_buf, r.sem_local.at[6])
    sources = (r.attn_k, r.attn_q, r.attn_v)
    alls = (r.k_all, r.q_all, r.v_all)
    seqs = (r.k_seq, r.q_seq, r.v_seq)
    own_slot = pair_at(turn * heads + head)
    fetch_own = [
        local(sources[i].at[:, :, cols(head)], alls[i].at[own_slot], r.sem_local.at[7 + i])
        for i in range(3)
    ]
    for c in fetch_hy:
        c.start()
    fetch_dy.start()
    fetch_w.start()

    def in_copy(i, d, arriving):
        to = (head + d) % heads
        source = (head - d + heads) % heads if arriving else head
        slot = pair_at(turn * heads + source)
        return remote(
            sources[i].at[:, :, cols(to)],
            alls[i].at[slot],
            r.sem_in_s.at[i, d],
            r.sem_in_r.at[i, d],
            to * share + turn,
        )

    for i in range(2):
        loop(1, heads, lambda d, i=i: in_copy(i, d, False).start())
    for c in fetch_own:
        c.start()
    fetch_o.start()
    fetch_rest = []
    for d in range(1, p.parts):
        c = local(r.weight.at[:, part_cols(d)], r.w_rest.at[d - 1], r.sem_rest.at[d - 1])
        fetch_rest.append(c)

    for c in fetch_hy:
        c.wait()
    lane_shape = (p.modes, tok)
    lag = lax.broadcasted_iota(jnp.int32, lane_shape, 1).astype(F32)

    def hy_block(i, g):
        return r.hy_in[i, :, rows_at(g, p.size)].astype(F32)

    def twice(x):
        return jnp.concatenate(split(x), axis=1)

    def state_of(decay, prod):
        both = dot_nn(jnp.concatenate(split(decay), axis=0), twice(prod))
        both = both[: p.modes] + both[p.modes :]
        return both[:, : p.size] + both[:, p.size :]

    def one_state(g):
        rate = column(r.rate, g)
        tail = jnp.exp(-rate * (tok - 1 - lag))
        first = jnp.exp(-rate * lag)
        lines = rows_at(g, p.modes)
        r.st_own[0, lines, :] = state_of(tail, hy_block(1, g) * hy_block(2, g)).astype(BF16)
        r.st_own[1, lines, :] = state_of(first, hy_block(0, g) * hy_block(3, g)).astype(BF16)

    loop(0, p.groups, one_state)

    near, far = p.near, p.far
    my_near, my_far = me % near, me // near

    def near_copy(d, arriving):
        source = (my_near - d + near) % near if arriving else my_near
        return remote(
            r.st_own,
            r.st_got.at[source],
            r.sem_st_s.at[d],
            r.sem_st_r.at[d],
            my_far * near + (my_near + d) % near,
        )

    loop(1, near, lambda d: near_copy(d, False).start())

    fetch_dy.wait()
    fetch_w.wait()
    for c in fetch_rest:
        c.start()

    def own_product(n):
        at_cols = rows_at(n, p.tile)
        r.g_part[:, at_cols] = dot_nt(r.dy_own[...], r.w_own[at_cols, :])

    loop(0, p.feat // p.tile, own_product)

    def place_of(flat):
        source, h = flat // (2 * heads), flat // 2 % heads
        return r.places[(h * share + source) * 2 + flat % 2]

    def find(place):
        slot = jnp.int32(0)
        for stored in range(2 * count):
            c, b = divmod(stored, 2)
            flat = c % share * heads + c // share
            slot = jnp.where(r.places[stored] == place, 2 * flat + b, slot)
        r.table[0, place] = slot
        r.table[1, place] = slot % 2 * count + slot // 2

    loop(0, 2 * count, find)

    row_id = lax.broadcasted_iota(jnp.int32, (8, tok), 0)
    empty = jnp.where(row_id == 0, NEG_LARGE, 0.0)

    def clear(n):
        r.ml[n] = empty

    loop(0, heads * count, clear)

    def hand_on(i, d, s, arriving):
        source = (turn - s + share) % share if arriving else turn
        slot = pair_at(source * heads + (head - d + heads) % heads)
        return remote(
            alls[i].at[slot],
            alls[i].at[slot],
            r.sem_fw_s.at[i, d, s],
            r.sem_fw_r.at[i, d, s],
            head * share + (turn + s) % share,
        )

    def arrive(*kinds):
        for i in kinds:
            fetch_own[i].wait()
            for s in range(1, share):
                hand_on(i, 0, s, False).start()

        def one(d):
            for i in kinds:
                in_copy(i, d, True).wait_recv()
                for s in range(1, share):
                    hand_on(i, d, s, False).start()

        loop(1, heads, one)

    def in_order(source, target, row):
        def one(place):
            target[rows_at(place, half), :] = source[r.table[row, place]]

        loop(0, 2 * count, one)

    def settle(i):
        for s in range(1, share):
            loop(0, heads, lambda d, s=s: hand_on(i, d, s, True).wait_recv())
        in_order(alls[i], seqs[i], 0)

    def g_place(n, source):
        slot, start = divmod(n * p.piece, half)
        return slot * count + turn * heads + source, pl.ds(start, p.piece)

    def g_copy(n, d, arriving):
        to = (head + d) % heads
        source = (head - d + heads) % heads if arriving else head
        rows = pl.ds(n * p.piece, p.piece)
        slot, inner = g_place(n, source)
        return remote(
            r.g_low.at[rows, cols(to)],
            r.g_all.at[slot, inner, :],
            r.sem_g_s.at[n, d],
            r.sem_g_r.at[n, d],
            to * share + turn,
        )

    def g_chunks(start, stop):
        for n in range(start, stop):
            for d in range(1, p.parts):
                dy_copy(d, n).wait_recv()
        rows = pl.ds(start * p.piece, (stop - start) * p.piece)

        def tile(c):
            at_cols = rows_at(c, p.tile)
            total = r.g_part[rows, at_cols]
            for d in range(1, p.parts):
                total = total + dot_nt(r.dy_got[d - 1, rows, :], r.w_rest[d - 1, at_cols, :])
            r.g_low[rows, at_cols] = total.astype(BF16)

        loop(0, p.feat // p.tile, tile)
        for n in range(start, stop):
            loop(1, heads, lambda d, n=n: g_copy(n, d, False).start())
        for n in range(start, stop):
            slot, inner = g_place(n, head)
            r.g_all[slot, inner, :] = r.g_low[pl.ds(n * p.piece, p.piece), cols(head)]

    def g_hand(n, s, arriving):
        source = (turn - s + share) % share if arriving else turn
        slot, start = divmod(n * p.piece, half)
        part = r.g_all.at[
            pl.ds(slot * count + source * heads, heads), pl.ds(start, p.piece), :
        ]
        return remote(
            part,
            part,
            r.sem_gf_s.at[n, s],
            r.sem_gf_r.at[n, s],
            head * share + (turn + s) % share,
        )

    def g_arrive(n):
        loop(1, heads, lambda d: g_copy(n, d, True).wait_recv())
        for s in range(1, share):
            g_hand(n, s, False).start()

    ones = jnp.ones((8, HD), BF16)

    def delta_copy(b, d, arriving):
        to = (head + d) % heads
        source = (head - d + heads) % heads if arriving else head
        return remote(
            r.delta_out.at[b, to],
            r.delta_all.at[b * count + turn * heads + source],
            r.sem_d_s.at[b, d],
            r.sem_d_r.at[b, d],
            to * share + turn,
        )

    def delta_half(b):
        rows = pl.ds(b * half, half)

        def one(h):
            prod = r.g_low[rows, cols(h)].astype(F32) * r.o_buf[rows, cols(h)].astype(F32)
            high, low = split(prod)
            r.delta_out[b, h] = dot_nt(ones, high) + dot_nt(ones, low)

        for h in range(heads):
            one(h)
        loop(1, heads, lambda d: delta_copy(b, d, False).start())
        r.delta_all[b * count + turn * heads + head] = r.delta_out[b, head]

    def delta_hand(b, s, arriving):
        source = (turn - s + share) % share if arriving else turn
        part = r.delta_all.at[pl.ds(b * count + source * heads, heads)]
        return remote(
            part,
            part,
            r.sem_df_s.at[b, s],
            r.sem_df_r.at[b, s],
            head * share + (turn + s) % share,
        )

    def delta_arrive(b):
        loop(1, heads, lambda d: delta_copy(b, d, True).wait_recv())
        for s in range(1, share):
            delta_hand(b, s, False).start()

    square = (tok, tok)

    def turn_keys(n):
        mine = p.own(n, turn)
        r.k_turn[n] = r.k_seq[rows_at(mine, tok), :].astype(F32).T.astype(BF16)

    def spread(n):
        mine = p.own(n, turn)
        first = p.offset(n, turn)
        keys = rows_at(mine, tok)

        def one(i, masked=False):
            s = dot_nt(r.k_seq[keys, :], r.q_seq[rows_at(i, tok), :])
            if masked:
                key_id = lax.broadcasted_iota(jnp.int32, square, 0)
                query_id = lax.broadcasted_iota(jnp.int32, square, 1)
                s = jnp.where(key_id <= query_id, s, NEG_LARGE)
            peak = jnp.max(s, axis=0, keepdims=True)
            e = jnp.exp2((s - peak) * LN2_SCALE)
            r.cache[first + i - mine] = e.astype(BF16)
            r.ml[n * count + i, 0:1, :] = peak
            r.ml[n * count + i, 1:2, :] = jnp.sum(e, axis=0, keepdims=True)

        def some(i, width, carry):
            for u in range(width):
                one(i + u)
            return carry

        one(mine, True)
        spans(mine + 1, count, some)

    def combine(i):
        peaks = [r.ml[n * count + i, 0:1, :] for n in range(heads)]
        peak = functools.reduce(jnp.maximum, peaks)
        total = 0.0
        for n in range(heads):
            weight = jnp.exp2((peaks[n] - peak) * LN2_SCALE)
            total = total + weight * r.ml[n * count + i, 1:2, :]
        r.ml_own[i] = empty
        r.ml_own[i, 0:1, :] = peak
        r.ml_own[i, 1:2, :] = total

    def ml_copy(s):
        return remote(
            r.ml_own,
            r.ml_got.at[s - 1],
            r.sem_ml_s.at[s],
            r.sem_ml_r.at[s],
            head * share + (turn + s) % share,
        )

    def join(i):
        peaks = [r.ml_own[i, 0:1, :]] + [r.ml_got[s, i, 0:1, :] for s in range(share - 1)]
        peak = functools.reduce(jnp.maximum, peaks)
        total = jnp.exp2((peaks[0] - peak) * LN2_SCALE) * r.ml_own[i, 1:2, :]
        for s in range(share - 1):
            weight = jnp.exp2((peaks[s + 1] - peak) * LN2_SCALE)
            total = total + weight * r.ml_got[s, i, 1:2, :]
        r.ml_own[i, 0:1, :] = peak
        r.ml_own[i, 1:2, :] = 1.0 / total

    def normal(n):
        mine = p.own(n, turn)
        first = p.offset(n, turn)

        def one(i):
            weight = jnp.exp2((r.ml[n * count + i, 0:1, :] - r.ml_own[i, 0:1, :]) * LN2_SCALE)
            weight = weight * r.ml_own[i, 1:2, :]
            e = r.cache[first + i - mine].astype(F32)
            r.cache[first + i - mine] = (e * weight).astype(BF16)

        loop(mine, count, one)

    def decay(rate, steps, good):
        power = jnp.exp(-rate * (tok * jnp.maximum(steps, 0)).astype(F32))
        return jnp.where(good, power, 0.0)

    def near_sum(g):
        rate = column(r.rate, g)
        lines = rows_at(g, p.modes)
        zero = jnp.zeros((p.modes, p.size), F32)
        total, back, fin, fin_back = zero, zero, zero, zero
        for other in range(near):
            ahead = r.st_got[other, 0, lines, :].astype(F32)
            behind = r.st_got[other, 1, lines, :].astype(F32)
            total = total + decay(rate, jnp.int32(near - 1 - other), True) * ahead
            back = back + decay(rate, jnp.int32(other), True) * behind
            gap = my_near - 1 - other
            fin = fin + decay(rate, gap, gap >= 0) * ahead
            gap = other - 1 - my_near
            fin_back = fin_back + decay(rate, gap, gap >= 0) * behind
        r.st_far[0, lines, :] = total.astype(BF16)
        r.st_far[1, lines, :] = back.astype(BF16)
        r.st_fin[0, lines, :] = fin
        r.st_fin[1, lines, :] = fin_back

    def far_copy(d):
        to = (my_far + d) % far
        return remote(
            r.st_far.at[(my_far + d) // far],
            r.far_got.at[d - 1],
            r.sem_far_s.at[d],
            r.sem_far_r.at[d],
            to * near + my_near,
        )

    def far_sum(g):
        rate = column(r.rate, g)
        lines = rows_at(g, p.modes)
        ahead = jnp.zeros((p.modes, p.size), F32)
        behind = ahead
        for d in range(1, far):
            got = r.far_got[d - 1, lines, :].astype(F32)
            source = (my_far - d + far) % far
            gap = (my_far - 1 - source) * near + my_near
            ahead = ahead + decay(rate, gap, source < my_far) * got
            gap = (source - 1 - my_far) * near + near - 1 - my_near
            behind = behind + decay(rate, gap, source > my_far) * got
        r.st_fin[0, lines, :] += ahead
        r.st_fin[1, lines, :] += behind

    lag_id = lax.broadcasted_iota(jnp.int32, lane_shape, 1)
    turned = jnp.where(lag_id == 0, 0, tok - lag_id).astype(F32)
    tall = (half, tok)
    row = lax.broadcasted_iota(jnp.int32, (half, half), 0)
    col = lax.broadcasted_iota(jnp.int32, (half, half), 1)
    blank = jnp.zeros((half, half), F32)

    def mixed(bands, prod, edge, state):
        high, low = split(bands)
        pair = twice(prod)
        out = dot_nn(high, pair) + dot_nn(low, pair)
        e_high = edge.astype(BF16).astype(F32)
        s_high, s_low = split(state)
        left = jnp.concatenate([e_high, edge - e_high, e_high], axis=0).T.astype(BF16)
        right = jnp.concatenate([s_high, s_high, s_low], axis=0)
        return out[:, : p.size] + out[:, p.size :] + dot_nn(left, right)

    def mix(g):
        rate = jnp.broadcast_to(column(r.rate, g), lane_shape)
        res = jnp.broadcast_to(column(r.res, g), lane_shape)
        taps = jnp.sum(res * jnp.exp(-rate * lag), axis=0, keepdims=True)
        back_taps = jnp.sum(res * jnp.exp(-rate * turned), axis=0, keepdims=True)
        lower = pltpu.roll(jnp.broadcast_to(back_taps, tall), 0, 1, stride=1, stride_axis=0)
        upper = pltpu.roll(jnp.broadcast_to(taps, tall), 0, 1, stride=1, stride_axis=0)
        near_low = jnp.where(col <= row, lower[:, :half], 0.0)
        near_up = jnp.where(col >= row, upper[:, :half], 0.0)
        lower = jnp.concatenate(
            [
                jnp.concatenate([near_low, blank], axis=1),
                jnp.concatenate([lower[:, half:], near_low], axis=1),
            ],
            axis=0,
        )
        upper = jnp.concatenate(
            [
                jnp.concatenate([near_up, upper[:, half:]], axis=1),
                jnp.concatenate([blank, near_up], axis=1),
            ],
            axis=0,
        )
        lines = rows_at(g, p.modes)
        into = res * jnp.exp(-rate * (lag + 1.0))
        back = res * jnp.exp(-rate * (tok - lag))
        k, v, dy = hy_block(1, g), hy_block(2, g), hy_block(3, g)
        conv = mixed(lower, k * v, into, r.st_fin[0, lines, :])
        mid = mixed(upper, hy_block(0, g) * dy, back, r.st_fin[1, lines, :])
        here = rows_at(g, p.size)
        r.hy_out[0, :, here] = (dy * conv).astype(BF16)
        r.hy_out[1, :, here] = (mid * v).astype(BF16)
        r.hy_out[2, :, here] = (mid * k).astype(BF16)

    hy_outs = (r.out_hq, r.out_hk, r.out_hv)
    give = [local(r.hy_out.at[i], hy_outs[i], r.sem_out.at[3 + i]) for i in range(3)]

    arrive(0, 1)
    loop(1, heads, lambda d: in_copy(2, d, False).start())
    settle(0)
    settle(1)
    loop(0, heads, turn_keys)
    loop(0, heads, spread)
    loop(0, count, combine)
    for s in range(1, share):
        ml_copy(s).start()
    for c in fetch_rest:
        c.wait()
    last = p.chunks - 1
    g_chunks(0, last)
    fetch_o.wait()
    delta_half(0)
    arrive(2)
    for s in range(1, share):
        ml_copy(s).wait_recv()
        ml_copy(s).wait_send()
    loop(0, count, join)
    loop(0, heads, normal)
    g_chunks(last, p.chunks)
    delta_half(1)
    loop(1, near, lambda d: near_copy(d, True).wait_recv())
    r.st_got[my_near] = r.st_own[...]
    loop(0, p.groups, near_sum)
    loop(1, far, lambda d: far_copy(d).start())
    settle(2)
    for n in range(last):
        g_arrive(n)
    delta_arrive(0)
    g_arrive(last)
    delta_arrive(1)
    for s in range(1, share):
        for n in range(p.chunks):
            g_hand(n, s, True).wait_recv()
        for b in range(2):
            delta_hand(b, s, True).wait_recv()
    in_order(r.g_all, r.g_seq, 1)

    def order_delta(i):
        for b in range(2):
            r.delta_row[i, :, b * half : (b + 1) * half] = r.delta_all[r.table[1, 2 * i + b]]

    loop(0, count, order_delta)

    def keep(kind, n, target, value):
        mine = p.own(n, turn)
        target[2 * mine] = value[:half]
        target[2 * mine + 1] = value[half:]
        for s in range(1, share):
            kv_copy(kind, n, s, target, False).start()

    def value_pass(n):
        mine = p.own(n, turn)
        first = p.offset(n, turn) - mine

        def some(i, width, acc):
            probs = jnp.concatenate([r.cache[first + i + u] for u in range(width)], axis=1)
            return acc + dot_nn(probs, r.g_seq[pl.ds(pl.multiple_of(i * tok, tok), width * tok), :])

        acc = spans(mine, count, some, jnp.zeros((tok, HD), F32))
        keep(0, n, r.dv_seq, acc.astype(BF16))

    def kv_copy(kind, n, s, target, arriving):
        source = (turn - s + share) % share if arriving else turn
        rows = pair_at(p.own(n, source))
        return remote(
            target.at[rows],
            target.at[rows],
            r.sem_kv_s.at[kind, n, s],
            r.sem_kv_r.at[kind, n, s],
            head * share + (turn + s) % share,
        )

    def kv_arrive(kind, target):
        def one(n):
            for s in range(1, share):
                kv_copy(kind, n, s, target, True).wait_recv()

        loop(0, heads, one)

    outs = (r.out_q, r.out_k, r.out_v)

    def res_copy(kind, d):
        to = (head + d) % heads
        return remote(
            r.send.at[kind, d],
            outs[kind].at[:, :, cols(head)],
            r.sem_res_s.at[kind, d],
            r.sem_res_r.at[kind, d],
            to * share + turn,
        )

    def res_local(kind):
        return local(r.send.at[kind, 0], outs[kind].at[:, :, cols(head)], r.sem_out.at[kind])

    def hand_back(kind, value_of):
        def one(d):
            flat = (turn * heads + (head + d) % heads) * 2
            for b in range(2):
                place = place_of(flat + b)
                value = value_of(place, (head + d) % heads, b)
                r.send[kind, d, b] = value

        def both(d):
            one(d)
            res_copy(kind, d).start()

        loop(1, heads, both)
        one(0)
        res_local(kind).start()

    loop(0, heads, value_pass)
    kv_arrive(0, r.dv_seq)
    hand_back(2, lambda place, h, b: r.dv_seq[place])

    def score_pass(n):
        mine = p.own(n, turn)
        first = p.offset(n, turn) - mine
        keys = rows_at(mine, tok)

        def some(i, width, acc):
            scores = []
            for u in range(width):
                grad_prob = dot_nt(r.v_seq[keys, :], r.g_seq[rows_at(i + u, tok), :])
                change = grad_prob - r.delta_row[i + u, 0:1, :]
                score = (r.cache[first + i + u].astype(F32) * change).astype(BF16)
                r.cache[first + i + u] = score
                scores.append(score)
            queries = r.q_seq[pl.ds(pl.multiple_of(i * tok, tok), width * tok), :]
            return acc + dot_nn(jnp.concatenate(scores, axis=1), queries)

        acc = spans(mine, count, some, jnp.zeros((tok, HD), F32))
        keep(1, n, r.dk_seq, (acc * SCALE).astype(BF16))

    loop(0, heads, score_pass)
    kv_arrive(1, r.dk_seq)
    hand_back(1, lambda place, h, b: r.dk_seq[place])

    def query_pass(t):
        pair = (2 * t, 2 * t + 1)
        both = p.held(pair[0], turn)

        def some(n, width, accs, queries=pair):
            spots = [p.offset(n + u, turn) - p.own(n + u, turn) for u in range(width)]
            left = jnp.concatenate([r.k_turn[n + u] for u in range(width)], axis=1)
            out = []
            for acc, i in zip(accs, queries, strict=True):
                right = jnp.concatenate([r.cache[spot + i] for spot in spots], axis=0)
                out.append(acc + dot_nn(left, right))
            return tuple(out)

        zero = jnp.zeros((HD, tok), F32)
        one, two = spans(0, both, some, (zero, zero))
        (two,) = lax.fori_loop(
            both, p.held(pair[1], turn), lambda n, c: some(n, 1, c, pair[1:]), (two,)
        )
        for i, acc in zip(pair, (one, two), strict=True):
            value = acc.T * SCALE
            r.dq_seq[2 * i] = value[:half]
            r.dq_seq[2 * i + 1] = value[half:]

    loop(0, count // 2, query_pass)

    def q_copy(s):
        return remote(
            r.dq_out.at[s - 1],
            r.dq_got.at[s - 1],
            r.sem_q_s.at[s],
            r.sem_q_r.at[s],
            head * share + (turn + s) % share,
        )

    for s in range(1, share):

        def pick(f, s=s):
            place = place_of((turn + s) % share * heads * 2 + f)
            r.dq_out[s - 1, f] = r.dq_seq[place].astype(BF16)

        loop(0, 2 * heads, pick)
        q_copy(s).start()

    loop(1, far, lambda d: far_copy(d).wait_recv())
    loop(0, p.groups, far_sum)
    loop(0, p.groups // 4, mix)
    for s in range(1, share):
        q_copy(s).wait_recv()

    def dq_value(place, h, b):
        value = r.dq_seq[place]
        for s in range(1, share):
            value = value + r.dq_got[s - 1, 2 * h + b].astype(F32)
        return value.astype(BF16)

    hand_back(0, dq_value)
    loop(p.groups // 4, p.groups, mix)
    for c in give:
        c.start()

    for n in range(p.chunks):
        for d in range(1, p.parts):
            dy_copy(d, n).wait_send()
    loop(1, near, lambda d: near_copy(d, False).wait_send())
    loop(1, far, lambda d: far_copy(d).wait_send())
    for i in range(3):
        loop(1, heads, lambda d, i=i: in_copy(i, d, False).wait_send())
        for s in range(1, share):
            loop(0, heads, lambda d, i=i, s=s: hand_on(i, d, s, False).wait_send())
    for n in range(p.chunks):
        loop(1, heads, lambda d, n=n: g_copy(n, d, False).wait_send())
    for b in range(2):
        loop(1, heads, lambda d, b=b: delta_copy(b, d, False).wait_send())
    for s in range(1, share):
        for n in range(p.chunks):
            g_hand(n, s, False).wait_send()
        for b in range(2):
            delta_hand(b, s, False).wait_send()
        q_copy(s).wait_send()

        def kv_sent(n, s=s):
            kv_copy(0, n, s, r.dv_seq, False).wait_send()
            kv_copy(1, n, s, r.dk_seq, False).wait_send()

        loop(0, heads, kv_sent)
    for kind in range(3):
        loop(1, heads, lambda d, kind=kind: res_copy(kind, d).wait_send())
        loop(1, heads, lambda d, kind=kind: res_copy(kind, d).wait_recv())
        res_local(kind).wait()
    for c in give:
        c.wait()


def copy_kernel(*refs):
    sources, targets, held, (sem_in, sem_out) = refs[:6], refs[6:12], refs[12:18], refs[18:]
    into, out = [], []
    for i in range(6):
        size = held[i].shape[0] // 2
        for j in range(2):
            part = pl.ds(j * size, size)
            into.append(
                pltpu.make_async_copy(sources[i].at[part], held[i].at[part], sem_in.at[i, j])
            )
            out.append(
                pltpu.make_async_copy(held[i].at[part], targets[i].at[part], sem_out.at[i, j])
            )
    for c in into:
        c.start()
    for c, d in zip(into, out, strict=True):
        c.wait()
        d.start()
    for d in out:
        d.wait()


def body(
    attn_q,
    attn_k,
    attn_v,
    attn_o,
    attn_dy,
    out_weight,
    block_place,
    hyena_q,
    hyena_k,
    hyena_v,
    hyena_dy,
    filter_residue,
    filter_rate,
):
    tok, feat = attn_q.shape
    chan = hyena_q.shape[1]
    modes, groups = filter_rate.shape
    count, parts = lax.axis_size("ctx"), lax.axis_size("tp")
    p = Plan(count, parts, tok, feat, attn_dy.shape[1], chan, modes, groups)
    items = scratch(p)
    names = INPUTS + OUTPUTS + tuple(items)
    hbm = pl.BlockSpec(memory_space=pl.ANY)
    vmem = pl.BlockSpec(memory_space=pltpu.VMEM)
    attn_out = jax.ShapeDtypeStruct((2, p.half, feat), BF16)
    hy_out = jax.ShapeDtypeStruct((tok, chan), BF16)
    outs = pl.pallas_call(
        functools.partial(kernel, p, names),
        in_specs=[pl.BlockSpec(memory_space=pltpu.SMEM), vmem, vmem] + [hbm] * 10,
        out_specs=[hbm] * 6,
        out_shape=[attn_out] * 3 + [hy_out] * 3,
        scratch_shapes=list(items.values()),
        compiler_params=pltpu.CompilerParams(
            collective_id=0, has_side_effects=True, vmem_limit_bytes=63 * 1024 * 1024
        ),
        name="grads",
    )(
        block_place,
        filter_rate,
        filter_residue,
        attn_q.reshape(2, p.half, feat),
        attn_k.reshape(2, p.half, feat),
        attn_v.reshape(2, p.half, feat),
        attn_o,
        attn_dy,
        out_weight,
        hyena_q,
        hyena_k,
        hyena_v,
        hyena_dy,
    )
    outs = pl.pallas_call(
        copy_kernel,
        in_specs=[hbm] * 6,
        out_specs=[hbm] * 6,
        out_shape=[attn_out] * 3 + [hy_out] * 3,
        scratch_shapes=[pltpu.VMEM(attn_out.shape, BF16)] * 3
        + [pltpu.VMEM(hy_out.shape, BF16)] * 3
        + [pltpu.SemaphoreType.DMA((6, 2))] * 2,
        name="results",
    )(*outs)
    return tuple(x.reshape(tok, feat) for x in outs[:3]) + tuple(outs[3:])


def solution(mesh):
    both = P("ctx", "tp")
    in_specs = (both,) * 5 + (P("tp", None), P()) + (both,) * 4 + (P(None, "tp"),) * 2
    return jax.shard_map(body, mesh=mesh, in_specs=in_specs, out_specs=(both,) * 6, check_vma=False)
```
